128 devices in a mesh: row: 16 (over z, x), col: 8 (over y, core).
Axes of the slice: x: 4, y: 4, z: 4, core: 2. Of those that a mesh axis runs over, the one named last changes fastest.
Arguments:
- encoder_tokens: bfloat16 [128, 64, 1024], P(('row', 'col')), may hold values from -16 to 16
- pair_list: int32 [16, 8, 2, 2], P('row', 'col'), may hold values from 0 to 127, as said below
- pair_count: int32 [16, 8], P('row', 'col'), may hold values from 1 to 2, as said below
- embed_weight: bfloat16 [1024, 768], replicated, may hold values from -0.1875 to 0.1875
- self_gain: float32 [2, 768], replicated, may hold values from 0.25 to 1.75
- self_qkv: bfloat16 [2, 768, 2304], replicated, may hold values from -10 to 10
- self_out: bfloat16 [2, 768, 768], replicated, may hold values from -0.21875 to 0.21875
- cross_gain: float32 [2, 2, 768], replicated, may hold values from 0.25 to 1.75
- cross_qkv: bfloat16 [2, 768, 2304], replicated, may hold values from -10 to 10
- cross_out: bfloat16 [2, 768, 768], replicated, may hold values from -0.21875 to 0.21875
- mlp_gain: float32 [2, 768], replicated, may hold values from 0.25 to 1.75
- mlp_up: bfloat16 [2, 3072, 768], P(None, ('row', 'col')), may hold values from -0.21875 to 0.21875
- mlp_down: bfloat16 [2, 3072, 768], P(None, ('row', 'col')), may hold values from -0.109375 to 0.109375
- conf_weight: float32 [768], replicated, may hold values from -0.21875 to 0.21875
- head_weight: bfloat16 [768, 1024], replicated, may hold values from -0.21875 to 0.21875
Outputs:
- pointmap_features: bfloat16 [128, 64, 1024], P(('row', 'col'))
The draws below stay inside these ranges and needn't reach their ends.
Inputs may be any that keep to these rules, and one draw needn't show every extreme that they name: `pair_list`: entry [r, c, s] holds two different images: the first held by a device of mesh row r, the second by a device of mesh column c. The first 1 slots of device (r, c) hold that device's own images as first images, so every image is in some used slot. Entries of unused slots are valid indices and are ignored. `pair_count`: device (0, 0) uses all its slots.
All inputs are finite; a program needn't handle non-finite values.
Results may differ from the reference program's by a relative error of at most 0.022.
Values may be sent and summed in bfloat16 or wider, within the bound.
No kernel may reach another device: no remote copies, remote signals or barrier semaphores. Data moves between devices by JAX's collectives and lax.ppermute only.
A program may use at most 128 MiB of HBM per device.

```python
import math
import jax
import jax.numpy as jnp
from jax import lax

D_ENC = 1024
D_DEC = 768
HEADS = 12
MLP = 3072
HEAD_DIM = 64
HEAD_OUT = 1024
TOKENS = 64
IMG_DEV = 1
PAIR_CAP = 2
IMAGES = 128
N_ROW = 16
N_COL = 8


def draw_encoder_tokens(key, part):
    drawn = jnp.clip(jax.random.normal(key, (IMAGES, TOKENS, D_ENC), jnp.float32), -6.0, 6.0)
    return drawn.astype(jnp.bfloat16)


def drawn_qkv(key):
    matrix = jnp.clip(jax.random.normal(key, (2, D_DEC, 3 * D_DEC), jnp.float32), -6.0, 6.0) / math.sqrt(D_DEC)
    return matrix.astype(jnp.bfloat16)


def draw_self_qkv(key, part):
    return drawn_qkv(jax.random.fold_in(key, 21))


def draw_cross_qkv(key, part):
    return drawn_qkv(jax.random.fold_in(key, 22))


def make_pairs(key):
    drawn_key = jax.random.fold_in(key, 11)
    split_keys = jax.random.split(drawn_key, 6)
    full_shape = (N_ROW, N_COL, PAIR_CAP)
    row_ids = jnp.arange(N_ROW, dtype=jnp.int32)[:, None, None]
    col_ids = jnp.arange(N_COL, dtype=jnp.int32)[None, :, None]
    slot_ids = jnp.arange(PAIR_CAP, dtype=jnp.int32)[None, None, :]
    hub_col = jax.random.randint(split_keys[0], (N_ROW, 1, 1), 0, N_COL)
    hub_coin = jax.random.randint(split_keys[1], full_shape, 0, 4)
    other_col = jax.random.randint(split_keys[2], full_shape, 0, N_COL)
    own_slot = jnp.broadcast_to(slot_ids < IMG_DEV, full_shape)
    first_col = jnp.where(own_slot, jnp.broadcast_to(col_ids, full_shape), jnp.where(hub_coin < 3, jnp.broadcast_to(hub_col, full_shape), other_col))
    first_held = jnp.where(own_slot, jnp.broadcast_to(jnp.minimum(slot_ids, IMG_DEV - 1), full_shape), jax.random.randint(split_keys[3], full_shape, 0, IMG_DEV))
    first_ids = (row_ids * N_COL + first_col) * IMG_DEV + first_held
    second_row = (row_ids + 1 + jax.random.randint(split_keys[4], full_shape, 0, N_ROW - 1)) % N_ROW
    second_ids = (second_row * N_COL + col_ids) * IMG_DEV + jax.random.randint(split_keys[5], full_shape, 0, IMG_DEV)
    listed = jnp.stack([first_ids, second_ids], -1).astype(jnp.int32)
    used_count = jax.random.randint(jax.random.fold_in(drawn_key, 9), (N_ROW, N_COL), IMG_DEV, PAIR_CAP + 1)
    used_count = used_count.at[0, 0].set(PAIR_CAP)
    return (listed, used_count.astype(jnp.int32))


def draw_pair_list(key, part):
    return make_pairs(key)[0]


def draw_pair_count(key, part):
    return make_pairs(key)[1]


def shard_levels(stream_key, shape, shards, low, high):
    level, own = 1.0, jax.random.fold_in(stream_key, 6)
    for dim, blocks in shards:
        draws = jnp.exp(jax.random.uniform(jax.random.fold_in(own, dim), (blocks,), jnp.float32, low / len(shards), high / len(shards)))
        level = level * jnp.repeat(draws, shape[dim] // blocks).reshape([-1 if axis == dim else 1 for axis in range(len(shape))])
    return level


def centred(rng, dims, deviation, limit, cuts=(), kind=jnp.bfloat16):
    result = jax.random.normal(rng, dims, jnp.float32) * deviation
    if len(cuts) > 0:
        result = shard_levels(rng, dims, cuts, -0.22, 0.18) * result
    return jnp.clip(result, min=-limit, max=limit).astype(kind)


def setup_inputs(seed: int = 0) -> dict:
    keys = jax.random.split(jax.random.key(seed), 16)
    return {
        "encoder_tokens": draw_encoder_tokens(jax.random.fold_in(keys[15], 71), 0),
        "pair_list": draw_pair_list(jax.random.fold_in(keys[15], 71), 0),
        "pair_count": draw_pair_count(jax.random.fold_in(keys[15], 71), 0),
        "embed_weight": centred(keys[3], (D_ENC, D_DEC), D_ENC ** -0.5, 0.1875),
        "self_gain": jnp.clip(1.0 + 0.15 * jax.random.normal(keys[4], (2, D_DEC), jnp.float32), 0.25, 1.75),
        "self_qkv": draw_self_qkv(jax.random.fold_in(keys[15], 71), 0),
        "self_out": centred(keys[6], (2, D_DEC, D_DEC), D_DEC ** -0.5, 0.21875),
        "cross_gain": jnp.clip(1.0 + 0.15 * jax.random.normal(keys[7], (2, 2, D_DEC), jnp.float32), 0.25, 1.75),
        "cross_qkv": draw_cross_qkv(jax.random.fold_in(keys[15], 71), 0),
        "cross_out": centred(keys[9], (2, D_DEC, D_DEC), D_DEC ** -0.5, 0.21875),
        "mlp_gain": jnp.clip(1.0 + 0.15 * jax.random.normal(keys[10], (2, D_DEC), jnp.float32), 0.25, 1.75),
        "mlp_up": centred(keys[11], (2, MLP, D_DEC), D_DEC ** -0.5, 0.21875, ((1, 128),)),
        "mlp_down": centred(keys[12], (2, MLP, D_DEC), MLP ** -0.5, 0.109375, ((1, 128),)),
        "conf_weight": centred(keys[13], (D_DEC,), D_DEC ** -0.5, 0.21875, (), jnp.float32),
        "head_weight": centred(keys[14], (D_DEC, HEAD_OUT), D_DEC ** -0.5, 0.21875),
    }


NORM_EPSILON = 1e-05

def normalize(tokens_in, gain):
    values32 = tokens_in.astype(jnp.float32)
    center = lax.optimization_barrier(jnp.mean(values32, -1, keepdims=True))
    centered = values32 - center
    variance = lax.optimization_barrier(jnp.mean(centered * centered, -1, keepdims=True))
    return (centered * lax.rsqrt(variance + NORM_EPSILON) * gain).astype(jnp.bfloat16)

def product(tokens_in, matrix):
    return jnp.einsum('...d,de->...e', tokens_in.astype(jnp.float32), matrix.astype(jnp.float32))

def attend(queries, key_block, value_block):
    dims_in = queries.shape
    split_shape = dims_in[:-1] + (HEADS, HEAD_DIM)
    q_heads = queries.reshape(split_shape).astype(jnp.float32)
    k_heads = key_block.reshape(split_shape).astype(jnp.float32)
    v_heads = value_block.reshape(split_shape).astype(jnp.float32)
    scores = jnp.einsum('bthe,bshe->bhts', q_heads, k_heads) / math.sqrt(HEAD_DIM)
    highest = lax.optimization_barrier(jnp.max(scores, -1, keepdims=True))
    expo = jnp.exp(scores - highest)
    weights = (expo / lax.optimization_barrier(jnp.sum(expo, -1, keepdims=True))).astype(jnp.bfloat16)
    attended = jnp.einsum('bhts,bshe->bthe', weights.astype(jnp.float32), v_heads)
    return attended.astype(jnp.bfloat16).reshape(dims_in)

def decode_view(tokens_in, other_in, view_side, self_gain, self_qkv, self_out, cross_gain, cross_qkv, cross_out, mlp_gain, mlp_up, mlp_down):
    model_width = tokens_in.shape[-1]
    normed = normalize(tokens_in, self_gain[view_side])
    mixed_qkv = product(normed, self_qkv[view_side]).astype(jnp.bfloat16)
    attended = attend(mixed_qkv[..., :model_width], mixed_qkv[..., model_width:2 * model_width], mixed_qkv[..., 2 * model_width:])
    after_self = (tokens_in.astype(jnp.float32) + product(attended, self_out[view_side])).astype(jnp.bfloat16)
    query_in = normalize(after_self, cross_gain[view_side, 0])
    memory_in = normalize(other_in, cross_gain[view_side, 1])
    queries = product(query_in, cross_qkv[view_side][:, :model_width]).astype(jnp.bfloat16)
    memory = product(memory_in, cross_qkv[view_side][:, model_width:]).astype(jnp.bfloat16)
    attended = attend(queries, memory[..., :model_width], memory[..., model_width:])
    after_cross = (after_self.astype(jnp.float32) + product(attended, cross_out[view_side])).astype(jnp.bfloat16)
    mlp_in = normalize(after_cross, mlp_gain[view_side])
    hidden = jax.nn.gelu(product(mlp_in, mlp_up[view_side].T), approximate=False).astype(jnp.bfloat16)
    return (after_cross.astype(jnp.float32) + product(hidden, mlp_down[view_side])).astype(jnp.bfloat16)

def reference(encoder_tokens, pair_list, pair_count, embed_weight, self_gain, self_qkv, self_out, cross_gain, cross_qkv, cross_out, mlp_gain, mlp_up, mlp_down, conf_weight, head_weight):
    embedded = product(encoder_tokens, embed_weight).astype(jnp.bfloat16)
    pair_rows = pair_list.reshape(-1, 2).astype(jnp.int32)
    first_ids = pair_rows[:, 0]
    second_ids = pair_rows[:, 1]
    usable = (jnp.arange(PAIR_CAP, dtype=jnp.int32)[None, None, :] < pair_count[:, :, None]).reshape(-1).astype(jnp.float32)

    def one_pair(pair_index):
        first_tokens = lax.dynamic_index_in_dim(embedded, first_ids[pair_index], 0, keepdims=True)
        second_tokens = lax.dynamic_index_in_dim(embedded, second_ids[pair_index], 0, keepdims=True)
        decoded_first = decode_view(first_tokens, second_tokens, 0, self_gain, self_qkv, self_out, cross_gain, cross_qkv, cross_out, mlp_gain, mlp_up, mlp_down)
        decoded_second = decode_view(second_tokens, first_tokens, 1, self_gain, self_qkv, self_out, cross_gain, cross_qkv, cross_out, mlp_gain, mlp_up, mlp_down)
        return (decoded_first[0], decoded_second[0])
    decoded_first, decoded_second = lax.map(one_pair, jnp.arange(first_ids.shape[0], dtype=jnp.int32))

    def weighted_terms(decoded):
        decoded32 = decoded.astype(jnp.float32)
        confidence = 1.0 + jnp.exp(jnp.einsum('ptd,d->pt', decoded32, conf_weight.astype(jnp.float32)))
        confidence = confidence * usable[:, None]
        return (confidence[..., None] * decoded32, confidence)
    numer_first, weight_first = weighted_terms(decoded_first)
    numer_second, weight_second = weighted_terms(decoded_second)
    numerator = jax.ops.segment_sum(numer_first, first_ids, num_segments=IMAGES) + jax.ops.segment_sum(numer_second, second_ids, num_segments=IMAGES)
    denominator = jax.ops.segment_sum(weight_first, first_ids, num_segments=IMAGES) + jax.ops.segment_sum(weight_second, second_ids, num_segments=IMAGES)
    joined_tokens = (numerator / denominator[..., None]).astype(jnp.bfloat16)
    return product(joined_tokens, head_weight).astype(jnp.bfloat16)
```

```python
import functools

import jax
import jax.numpy as jnp
from jax import lax
from jax.experimental import pallas as pl
from jax.experimental.pallas import tpu as pltpu
from jax.sharding import PartitionSpec as P


HEADS = 12
HEAD_DIM = 64
NORM_EPSILON = 1e-05
D = 768
T = 64
SLOTS = 4
AUX = 128
MSG = D + AUX
F32 = jnp.float32
BF16 = jnp.bfloat16
AXES = ("row", "col")


def coords(i):
    return i // 32, (i // 8) % 4, (i // 2) % 4, i % 2


def linear(z, x, y, c):
    return ((z * 4 + x) * 4 + y) * 2 + c


Z, X, Y, C = 0, 1, 2, 3


def send(array, core0, core1):
    pairs = []
    for i in range(128):
        at = list(coords(i))
        for dim, mask in (core0, core1)[at[3]]:
            at[dim] ^= mask
        pairs.append((i, linear(*at)))
    return lax.ppermute(array, AXES, pairs)


def swap(array):
    return send(array, ((C, 1),), ((C, 1),))


def join(*arrays):
    return jnp.concatenate(arrays, axis=0)


def place(delta, order):
    found = jnp.int32(0)
    for at, mask in enumerate(order):
        found = jnp.where(delta == mask, at, found)
    return found


def coordinates(me):
    return me >> 5, (me >> 3) & 3, (me >> 1) & 3, me & 1


VMEM = pl.BlockSpec(memory_space=pltpu.VMEM)
SMEM = pl.BlockSpec(memory_space=pltpu.SMEM)
HBM = pl.BlockSpec(memory_space=pltpu.HBM)


def in_hbm(*arrays):
    return [pltpu.with_memory_space_constraint(a, pltpu.HBM) for a in arrays]


def seconds_at(ids_ref, z, x, core):
    found = []
    for second in (ids_ref[1], ids_ref[3]):
        to_z, to_x, _, _ = coordinates(second)
        last = jnp.where(core == 0, z ^ to_z, x ^ to_x)
        first = jnp.where(core == 0, x ^ to_x, z ^ to_z)
        found.append((last, (last & 1) * 4 + place(first, (0, 1, 3, 2))))
    return found


def pick_kernel(me_ref, far_ref, tokens, out_ref, sems):
    z, x, _, core = coordinates(me_ref[0])
    copies = [
        pltpu.make_async_copy(tokens.at[at], out_ref.at[n], sems.at[n])
        for n, (_, at) in enumerate(seconds_at(far_ref, z, x, core))
    ]
    for copy in copies:
        copy.start()
    for copy in copies:
        copy.wait()


def select_kernel(me_ref, mine_ref, theirs_ref, tokens, tokens_far, line, line_far, own, out_ref, sems):
    z, x, y, core = coordinates(me_ref[0])
    for n, (last, at) in enumerate(seconds_at(mine_ref, z, x, core)):

        @pl.when(last < 2)
        def _(n=n, at=at):
            pltpu.make_async_copy(tokens.at[at], out_ref.at[n], sems.at[n]).start()

        @pl.when(last >= 2)
        def _(n=n):
            pltpu.make_async_copy(tokens_far.at[n], out_ref.at[n], sems.at[n]).start()

    for n, first in ((2, mine_ref[2]), (3, theirs_ref[2])):
        delta = y ^ ((first >> 1) & 3)
        at = jnp.where(core == 0, place(delta, (0, 1, 3, 2)), place(delta, (0, 3, 1, 2)))

        @pl.when(at < 2)
        def _(n=n, at=at):
            pltpu.make_async_copy(line.at[at, pl.ds(96, T)], out_ref.at[n], sems.at[n]).start()

        @pl.when(at >= 2)
        def _(n=n, at=at):
            pltpu.make_async_copy(line_far.at[at - 2, pl.ds(96, T)], out_ref.at[n], sems.at[n]).start()

    out_ref[4] = own[...]
    for n in range(4):
        pltpu.make_async_copy(own, out_ref.at[n], sems.at[n]).wait()


def normed(values, gain):
    values = values.astype(F32)
    centered = values - jnp.mean(values, -1, keepdims=True)
    variance = jnp.mean(centered * centered, -1, keepdims=True)
    return (centered * lax.rsqrt(variance + NORM_EPSILON) * gain).astype(BF16)


def matmul(a, b):
    return lax.dot_general(a, b, (((1,), (0,)), ((), ())), preferred_element_type=F32)


def attention(qkv_ref, score_ref, expo_ref, out_ref):
    pairs = HEADS // 2
    left = lax.broadcasted_iota(jnp.int32, (T, 128), 1) < HEAD_DIM
    same = (lax.broadcasted_iota(jnp.int32, (128, 128), 0) < HEAD_DIM) == (
        lax.broadcasted_iota(jnp.int32, (128, 128), 1) < HEAD_DIM
    )
    ones = jnp.where(same, 1.0, 0.0).astype(BF16)

    def rows_of(slot):
        return pl.ds(slot * T, T)

    def split(both):
        zero = jnp.zeros_like(both)
        return jnp.concatenate([jnp.where(left, both, zero), jnp.where(left, zero, both)], axis=0)

    def score(slot, carry):
        for pair in range(pairs):
            q = qkv_ref[rows_of(slot), pl.ds(pair * 128, 128)]
            k = split(qkv_ref[rows_of(slot), pl.ds(D + pair * 128, 128)])
            score_ref[slot * pairs + pair] = lax.dot_general(
                q, k, (((1,), (1,)), ((), ())), preferred_element_type=F32
            )
        return carry

    def exponent(slot, carry):
        for pair in range(pairs):
            scores = score_ref[slot * pairs + pair] * 0.125
            high_left = jnp.max(jnp.where(left, scores, -jnp.inf), 1, keepdims=True)
            high_right = jnp.max(jnp.where(left, -jnp.inf, scores), 1, keepdims=True)
            expo = jnp.exp(scores - jnp.where(left, high_left, high_right))
            expo_ref[slot * pairs + pair] = expo.astype(BF16)
        return carry

    def weigh(slot, carry):
        for pair in range(pairs):
            expo = expo_ref[slot * pairs + pair]
            v = split(qkv_ref[rows_of(slot), pl.ds(2 * D + pair * 128, 128)])
            out_ref[rows_of(slot), pl.ds(pair * 128, 128)] = (
                matmul(expo, v) * (1.0 / matmul(expo, ones))
            ).astype(BF16)
        return carry

    for stage in (score, exponent, weigh):
        for slot in range(SLOTS):
            stage(slot, 0)


ATT_SCRATCH = [
    pltpu.VMEM((SLOTS * T, D), BF16),
    pltpu.VMEM((SLOTS * T, D), BF16),
    pltpu.VMEM((SLOTS * T, 3 * D), BF16),
    pltpu.VMEM((SLOTS * T, D), BF16),
    pltpu.VMEM((SLOTS * HEADS // 2, T, 128), F32),
    pltpu.VMEM((SLOTS * HEADS // 2, T, 128), BF16),
    pltpu.VMEM((D, 3 * D), BF16),
    pltpu.VMEM((D, D), BF16),
    pltpu.VMEM((D, 3 * D), BF16),
    pltpu.VMEM((D, D), BF16),
    pltpu.SemaphoreType.DMA((4,)),
]


def attend_kernel(
    me_ref,
    mine_ref,
    theirs_ref,
    local_ref,
    recv_ref,
    self_gain_ref,
    cross_gain_ref,
    mlp_gain_ref,
    self_qkv_hbm,
    self_out_hbm,
    cross_qkv_hbm,
    cross_out_hbm,
    after_ref,
    mlp_in_ref,
    x_ref,
    y_ref,
    qkv_ref,
    att_ref,
    score_ref,
    expo_ref,
    self_qkv,
    self_out,
    cross_qkv,
    cross_out,
    sems,
):
    side = me_ref[0] & 1
    copies = [
        pltpu.make_async_copy(src.at[side], dst, sems.at[n])
        for n, (src, dst) in enumerate(
            (
                (self_qkv_hbm, self_qkv),
                (self_out_hbm, self_out),
                (cross_qkv_hbm, cross_qkv),
                (cross_out_hbm, cross_out),
            )
        )
    ]
    for copy in copies:
        copy.start()

    def place(first_ref, second_ref):
        first_ref[0:64] = local_ref[4]
        first_ref[64:128] = jnp.where((mine_ref[2] & 1) == side, local_ref[2], recv_ref[3])
        first_ref[128:192] = recv_ref[4]
        first_ref[192:256] = jnp.where((theirs_ref[2] & 1) == side, local_ref[3], recv_ref[2])
        second_ref[0:64] = local_ref[0]
        second_ref[64:128] = local_ref[1]
        second_ref[128:192] = recv_ref[0]
        second_ref[192:256] = recv_ref[1]

    @pl.when(side == 0)
    def _():
        place(x_ref, y_ref)

    @pl.when(side == 1)
    def _():
        place(y_ref, x_ref)

    xn = normed(x_ref[...], self_gain_ref[pl.ds(side, 1), :])
    copies[0].wait()
    qkv_ref[...] = matmul(xn, self_qkv[...]).astype(BF16)
    attention(qkv_ref, score_ref, expo_ref, att_ref)
    copies[1].wait()
    after_self = (x_ref[...].astype(F32) + matmul(att_ref[...], self_out[...])).astype(BF16)
    x_ref[...] = after_self
    qn = normed(after_self, cross_gain_ref[pl.ds(2 * side, 1), :])
    yn = normed(y_ref[...], cross_gain_ref[pl.ds(2 * side + 1, 1), :])
    copies[2].wait()
    qkv_ref[:, 0:D] = matmul(qn, cross_qkv[:, 0:D]).astype(BF16)
    qkv_ref[:, D : 3 * D] = matmul(yn, cross_qkv[:, D : 3 * D]).astype(BF16)
    attention(qkv_ref, score_ref, expo_ref, att_ref)
    copies[3].wait()
    after_cross = (x_ref[...].astype(F32) + matmul(att_ref[...], cross_out[...])).astype(BF16)
    after_ref[...] = after_cross
    mlp_in_ref[...] = normed(after_cross, mlp_gain_ref[pl.ds(side, 1), :])


def gelu(v):
    return v * (lax.erf(v * 0.7071067811865476) + 1.0) * 0.5


def accumulate(count, mlp_in_ref, weights, acc_ref, held, sems):
    copies = [pltpu.make_async_copy(weights[n], held.at[n], sems.at[n]) for n in range(count)]
    for copy in copies:
        copy.start()
    for n in range(count):
        copies[n].wait()
        up = held[n, :, 0].reshape(384, D)
        down = held[n, :, 1].reshape(384, D)
        lifted = lax.dot_general(
            mlp_in_ref[...], up, (((1,), (1,)), ((), ())), preferred_element_type=F32
        )
        acc_ref[...] += matmul(gelu(lifted).astype(BF16), down)


def mlp_kernel(count, after_ref, mlp_in_ref, *refs):
    acc_ref, held, sems = refs[count:]
    acc_ref[...] = after_ref[...].astype(F32)
    accumulate(count, mlp_in_ref, refs[:count], acc_ref, held, sems)


def mlp_last_kernel(count, me_ref, mine_ref, theirs_ref, before_ref, mlp_in_ref, conf_ref, *refs):
    keep_ref, swap_ref, a_ref, b_ref, acc_ref, message, held, sems = refs[count:]
    acc_ref[...] = before_ref[...]
    accumulate(count, mlp_in_ref, refs[:count], acc_ref, held, sems)
    decoded = acc_ref[...].astype(BF16)
    conf = 1.0 + jnp.exp(jnp.sum(decoded.astype(F32) * conf_ref[...], -1, keepdims=True))
    high = conf.astype(BF16)
    rest = conf - high.astype(F32)
    middle = rest.astype(BF16)
    low = (rest - middle.astype(F32)).astype(BF16)
    lane = lax.broadcasted_iota(jnp.int32, (T, AUX), 1)
    side = me_ref[0] & 1
    for slot in range(SLOTS):
        rows = slice(slot * T, slot * T + T)
        ids = (mine_ref, theirs_ref)[slot // 2]
        held_by = jnp.where(side == 0, ids[2 * (slot % 2)], ids[2 * (slot % 2) + 1])
        owner = jnp.where(slot % 2 < ids[4], held_by, -1).astype(F32)
        aux = jnp.where(lane == 0, owner, 0.0)
        aux = jnp.where(lane == 1, high[rows].astype(F32), aux)
        aux = jnp.where(lane == 2, middle[rows].astype(F32), aux)
        aux = jnp.where(lane == 3, low[rows].astype(F32), aux)
        message[slot, :, 0:D] = decoded[rows]
        message[slot, :, D:MSG] = aux.astype(BF16)

    def put(ref, slots):
        for n, slot in enumerate(slots):
            ref[n] = message[slot]

    @pl.when(side == 0)
    def _():
        put(keep_ref, (0, 1, 3))
        put(swap_ref, (2, 1, 3))
        put(a_ref, (1, 3))
        put(b_ref, (1, 3))

    @pl.when(side == 1)
    def _():
        put(keep_ref, (0, 1, 1))
        put(swap_ref, (2, 3, 3))
        put(a_ref, (2, 3))
        put(b_ref, (0, 1))


def total_of(aux):
    return aux[:, 1:2] + aux[:, 2:3] + aux[:, 3:4]


def owner_of(ref, slot):
    lane = lax.broadcasted_iota(jnp.int32, (16, AUX), 1)
    aux = ref[slot, 0:16, D:MSG].astype(F32)
    return jnp.max(jnp.where(lane == 0, aux, -1.0)).astype(jnp.int32)


def add_to(sums, ref, slot):
    conf = total_of(ref[slot, :, D:MSG].astype(F32))
    sums[:, 0:D] += conf * ref[slot, :, 0:D].astype(F32)
    sums[:, D:MSG] += jnp.broadcast_to(conf, (T, AUX))


def middle_kernel(me_ref, keep, swapped, *refs):
    a, b = refs[0:3], refs[3:6]
    out_0 = refs[6]
    outs = refs[7:10]
    sums = refs[10]
    z, x, _, core = coordinates(me_ref[0])
    sums[0:4] = jnp.zeros((4, T, MSG), F32)

    def collect(messages):
        for ref, slot in messages:
            owner = owner_of(ref, slot)
            to_z, to_x, _, _ = coordinates(owner)
            here = jnp.where(core == 0, to_x == x, to_z == z)
            to = jnp.where(core == 0, to_z ^ z, to_x ^ x)
            add_to(sums.at[jnp.where((owner >= 0) & here, to, 4)], ref, slot)

    @pl.when(core == 0)
    def _():
        collect([(swapped, 0), (swapped, 1)] + [(r, slot) for r in a for slot in range(2)])

    @pl.when(core == 1)
    def _():
        collect([(keep, 0), (keep, 1)] + [(r, slot) for r in b for slot in range(2)])

    out_0[...] = sums[0]
    lane = lax.broadcasted_iota(jnp.int32, (T, AUX), 1)
    for mask, out in zip((1, 3, 2), outs):
        out[:, 0:D] = sums[mask, :, 0:D].astype(BF16)
        denominator = sums[mask, :, D:MSG]
        high = denominator.astype(BF16)
        rest = denominator - high.astype(F32)
        middle = rest.astype(BF16)
        low = rest - middle.astype(F32)
        aux = jnp.where(lane == 1, high.astype(F32), 0.0)
        aux = jnp.where(lane == 2, middle.astype(F32), aux)
        out[:, D:MSG] = jnp.where(lane == 3, low, aux).astype(BF16)


def row_kernel(me_ref, keep, swapped, *refs):
    a, b = refs[0:3], refs[3:6]
    sums = refs[6]
    me = me_ref[0]
    core = me & 1
    sums[...] = jnp.zeros((T, MSG), F32)

    def collect(messages):
        for ref, slot in messages:

            @pl.when(owner_of(ref, slot) == me)
            def _(ref=ref, slot=slot):
                add_to(sums, ref, slot)

    @pl.when(core == 0)
    def _():
        collect([(keep, n) for n in range(3)] + [(r, slot) for r in b for slot in range(2)])

    @pl.when(core == 1)
    def _():
        collect([(swapped, n) for n in range(3)] + [(r, slot) for r in a for slot in range(2)])


def final_kernel(column, row, from_1, from_3, from_2, head, out_ref):
    sums = column[...] + row[...]
    numerator, denominator = sums[:, 0:D], sums[:, D : D + 1]
    for piece in (from_1, from_3, from_2):
        numerator += piece[:, 0:D].astype(F32)
        denominator += total_of(piece[:, D:MSG].astype(F32))
    joined = (numerator / denominator).astype(BF16)
    out_ref[0] = matmul(joined, head[...]).astype(BF16)


def params(mib):
    return pltpu.CompilerParams(vmem_limit_bytes=mib * 2**20)


def shards(
    encoder_tokens,
    pair_list,
    pair_count,
    embed_weight,
    self_gain,
    self_qkv,
    self_out,
    cross_gain,
    cross_qkv,
    cross_out,
    mlp_gain,
    mlp_up,
    mlp_down,
    conf_weight,
    head_weight,
):
    me = lax.axis_index("row") * 8 + lax.axis_index("col")
    core = me & 1

    up_out, down_out = (lax.dynamic_index_in_dim(w, 1 - core, 0, False) for w in (mlp_up, mlp_down))
    came = swap(jnp.stack([up_out, down_out]))
    up_own, down_own = (lax.dynamic_index_in_dim(w, core, 0, False) for w in (mlp_up, mlp_down))
    mine = jnp.concatenate([pair_list.reshape(4), pair_count.reshape(1)])
    theirs = swap(mine)
    far = send(mine, ((Z, 3),), ((X, 3),))
    ids = (me.reshape(1), mine, theirs)

    own = jnp.einsum(
        "td,de->te", encoder_tokens[0], embed_weight, preferred_element_type=F32
    ).astype(BF16)

    block = jnp.concatenate([jnp.stack([up_own, down_own]), came], axis=1)
    block = join(block.reshape(96, D), own)[None]
    line = join(block, send(block, ((Y, 1),), ((Y, 3),)))
    line_far = send(line, ((Y, 3),), ((Y, 1),))

    def over_plane(held, first, last):
        near = send(held, ((first, 1),), ((first, 3),))
        held = join(held[:, :96], near[:, :96])
        held = join(held, send(held, ((first, 3),), ((first, 1),)))
        by_1 = send(held, ((last, 1),), ((last, 3),))
        by_3 = send(held, ((last, 3),), ((last, 1),))
        by_2 = send(by_1, ((last, 3),), ((last, 1),))
        return [h.reshape(8, 2, 48, D) for h in (held, by_1, by_3, by_2)]

    weights_a = over_plane(line, X, Z)
    weights_b = over_plane(line_far, Z, X)

    tokens = own[None]
    tokens = join(tokens, send(tokens, ((X, 1),), ((Z, 1),)))
    tokens = join(tokens, send(tokens, ((X, 3),), ((Z, 3),)))
    tokens = join(tokens, send(tokens, ((Z, 1),), ((X, 1),)))
    picked = pl.pallas_call(
        pick_kernel,
        out_shape=jax.ShapeDtypeStruct((2, T, D), BF16),
        in_specs=[SMEM] * 2 + [HBM],
        out_specs=VMEM,
        scratch_shapes=[pltpu.SemaphoreType.DMA((2,))],
        name="pick",
    )(ids[0], far, *in_hbm(tokens))
    tokens_far = send(picked, ((Z, 3),), ((X, 3),))
    selected = pl.pallas_call(
        select_kernel,
        out_shape=jax.ShapeDtypeStruct((5, T, D), BF16),
        in_specs=[SMEM] * 3 + [HBM] * 4 + [VMEM],
        out_specs=VMEM,
        scratch_shapes=[pltpu.SemaphoreType.DMA((4,))],
        name="select",
    )(*ids, *in_hbm(tokens, tokens_far, line, line_far), own)
    received = swap(selected)

    after, mlp_in = pl.pallas_call(
        attend_kernel,
        out_shape=[jax.ShapeDtypeStruct((SLOTS * T, D), BF16)] * 2,
        in_specs=[SMEM] * 3 + [VMEM] * 5 + [HBM] * 4,
        out_specs=[VMEM, VMEM],
        scratch_shapes=ATT_SCRATCH,
        compiler_params=params(32),
        name="attend",
    )(
        *ids,
        selected,
        received,
        self_gain,
        cross_gain.reshape(4, D),
        mlp_gain,
        *in_hbm(self_qkv, self_out, cross_qkv, cross_out),
    )

    def held_weights(count):
        return [pltpu.VMEM((count, 8, 2, 48, D), BF16), pltpu.SemaphoreType.DMA((count,))]

    sums = jax.ShapeDtypeStruct((SLOTS * T, D), F32)
    partial = pl.pallas_call(
        functools.partial(mlp_kernel, 6),
        out_shape=sums,
        in_specs=[VMEM] * 2 + [HBM] * 6,
        out_specs=VMEM,
        scratch_shapes=held_weights(6),
        compiler_params=params(32),
        name="lift",
    )(after, mlp_in, *weights_a[:3], *weights_b[:3])
    msg = lambda *shape: jax.ShapeDtypeStruct((*shape, MSG), BF16)
    keep, outgoing, piece_a, piece_b = pl.pallas_call(
        functools.partial(mlp_last_kernel, 2),
        out_shape=[msg(3, T), msg(3, T), msg(2, T), msg(2, T)],
        in_specs=[SMEM] * 3 + [VMEM] * 3 + [HBM] * 2,
        out_specs=[VMEM] * 4,
        scratch_shapes=[pltpu.VMEM((SLOTS * T, D), F32), pltpu.VMEM((SLOTS, T, MSG), BF16)]
        + held_weights(2),
        compiler_params=params(32),
        name="last",
    )(*ids, partial, mlp_in, conf_weight.reshape(1, D), weights_a[3], weights_b[3])

    incoming = swap(outgoing)
    masks = (1, 3, 2)
    got_a = [send(piece_a, ((Y, m), (C, 1)), ((X, m), (C, 1))) for m in masks]
    got_b = [send(piece_b, ((Y, m),), ((Z, m),)) for m in masks]
    summed = jax.ShapeDtypeStruct((T, MSG), F32)
    column, *parts = pl.pallas_call(
        middle_kernel,
        out_shape=[summed] + [msg(T)] * 3,
        in_specs=[SMEM] + [VMEM] * 8,
        out_specs=[VMEM] * 4,
        scratch_shapes=[pltpu.VMEM((5, T, MSG), F32)],
        name="middle",
    )(ids[0], keep, incoming, *got_a, *got_b)
    last = [send(s, ((Z, m),), ((X, m),)) for s, m in zip(parts, masks)]
    row = pl.pallas_call(
        row_kernel,
        out_shape=summed,
        in_specs=[SMEM] + [VMEM] * 8,
        out_specs=VMEM,
        name="rows",
    )(ids[0], keep, incoming, *got_a, *got_b)
    return pl.pallas_call(
        final_kernel,
        out_shape=jax.ShapeDtypeStruct((1, T, 1024), BF16),
        in_specs=[VMEM] * 6,
        out_specs=VMEM,
        name="head",
    )(column, row, *last, head_weight)


def solution(mesh):
    return jax.shard_map(
        shards,
        mesh=mesh,
        in_specs=(
            P(("row", "col"), None, None),
            P("row", "col", None, None),
            P("row", "col"),
            P(),
            P(),
            P(),
            P(),
            P(),
            P(),
            P(),
            P(),
            P(None, ("row", "col"), None),
            P(None, ("row", "col"), None),
            P(),
            P(),
        ),
        out_specs=P(("row", "col"), None, None),
        check_vma=False,
    )
```

```python
import functools

import jax
import jax.numpy as jnp
from jax import lax
from jax.experimental import pallas as pl
from jax.experimental.pallas import tpu as pltpu
from jax.sharding import PartitionSpec as P


HEADS = 12
HEAD_DIM = 64
NORM_EPSILON = 1e-05
D = 768
T = 64
SLOTS = 4
AUX = 128
MSG = D + AUX
F32 = jnp.float32
BF16 = jnp.bfloat16
AXES = ("row", "col")


def coords(i):
    return i // 32, (i // 8) % 4, (i // 2) % 4, i % 2


def linear(z, x, y, c):
    return ((z * 4 + x) * 4 + y) * 2 + c


Z, X, Y, C = 0, 1, 2, 3


def send(array, core0, core1):
    pairs = []
    for i in range(128):
        at = list(coords(i))
        for dim, mask in (core0, core1)[at[3]]:
            at[dim] ^= mask
        pairs.append((i, linear(*at)))
    return lax.ppermute(array, AXES, pairs)


def swap(array):
    return send(array, ((C, 1),), ((C, 1),))


def join(*arrays):
    return jnp.concatenate(arrays, axis=0)


def place(delta, order):
    found = jnp.int32(0)
    for at, mask in enumerate(order):
        found = jnp.where(delta == mask, at, found)
    return found


def coordinates(me):
    return me >> 5, (me >> 3) & 3, (me >> 1) & 3, me & 1


VMEM = pl.BlockSpec(memory_space=pltpu.VMEM)
SMEM = pl.BlockSpec(memory_space=pltpu.SMEM)
HBM = pl.BlockSpec(memory_space=pltpu.HBM)


def in_hbm(*arrays):
    return [pltpu.with_memory_space_constraint(a, pltpu.HBM) for a in arrays]


def seconds_at(ids_ref, z, x, core):
    found = []
    for second in (ids_ref[1], ids_ref[3]):
        to_z, to_x, _, _ = coordinates(second)
        last = jnp.where(core == 0, z ^ to_z, x ^ to_x)
        first = jnp.where(core == 0, x ^ to_x, z ^ to_z)
        found.append((last, (last >> 1) * 4 + place(first, (0, 1, 3, 2))))
    return found


def pick_kernel(me_ref, far_ref, tokens, out_ref, sems):
    z, x, _, core = coordinates(me_ref[0])
    copies = [
        pltpu.make_async_copy(tokens.at[at], out_ref.at[n], sems.at[n])
        for n, (_, at) in enumerate(seconds_at(far_ref, z, x, core))
    ]
    for copy in copies:
        copy.start()
    for copy in copies:
        copy.wait()


def select_kernel(me_ref, mine_ref, theirs_ref, tokens, tokens_far, line, line_far, own, out_ref, sems):
    z, x, y, core = coordinates(me_ref[0])
    for n, (last, at) in enumerate(seconds_at(mine_ref, z, x, core)):

        @pl.when((last == 0) | (last == 3))
        def _(n=n, at=at):
            pltpu.make_async_copy(tokens.at[at], out_ref.at[n], sems.at[n]).start()

        @pl.when((last == 1) | (last == 2))
        def _(n=n):
            pltpu.make_async_copy(tokens_far.at[n], out_ref.at[n], sems.at[n]).start()

    for n, first in ((2, mine_ref[2]), (3, theirs_ref[2])):
        delta = y ^ ((first >> 1) & 3)
        at = jnp.where(core == 0, place(delta, (0, 1, 3, 2)), place(delta, (0, 3, 1, 2)))

        @pl.when(at < 2)
        def _(n=n, at=at):
            pltpu.make_async_copy(line.at[at, pl.ds(96, T)], out_ref.at[n], sems.at[n]).start()

        @pl.when(at >= 2)
        def _(n=n, at=at):
            pltpu.make_async_copy(line_far.at[at - 2, pl.ds(96, T)], out_ref.at[n], sems.at[n]).start()

    out_ref[4] = own[...]
    for n in range(4):
        pltpu.make_async_copy(own, out_ref.at[n], sems.at[n]).wait()


def normed(values, gain):
    values = values.astype(F32)
    centered = values - jnp.mean(values, -1, keepdims=True)
    variance = jnp.mean(centered * centered, -1, keepdims=True)
    return (centered * lax.rsqrt(variance + NORM_EPSILON) * gain).astype(BF16)


def matmul(a, b):
    return lax.dot_general(a, b, (((1,), (0,)), ((), ())), preferred_element_type=F32)


def attention(qkv_ref, score_ref, expo_ref, out_ref):
    pairs = HEADS // 2
    left = lax.broadcasted_iota(jnp.int32, (T, 128), 1) < HEAD_DIM
    same = (lax.broadcasted_iota(jnp.int32, (128, 128), 0) < HEAD_DIM) == (
        lax.broadcasted_iota(jnp.int32, (128, 128), 1) < HEAD_DIM
    )
    ones = jnp.where(same, 1.0, 0.0).astype(BF16)

    def rows_of(slot):
        return pl.ds(slot * T, T)

    def split(both):
        zero = jnp.zeros_like(both)
        return jnp.concatenate([jnp.where(left, both, zero), jnp.where(left, zero, both)], axis=0)

    def score(slot, carry):
        for pair in range(pairs):
            q = qkv_ref[rows_of(slot), pl.ds(pair * 128, 128)]
            k = split(qkv_ref[rows_of(slot), pl.ds(D + pair * 128, 128)])
            score_ref[slot * pairs + pair] = lax.dot_general(
                q, k, (((1,), (1,)), ((), ())), preferred_element_type=F32
            )
        return carry

    def exponent(slot, carry):
        for pair in range(pairs):
            scores = score_ref[slot * pairs + pair] * 0.125
            high_left = jnp.max(jnp.where(left, scores, -jnp.inf), 1, keepdims=True)
            high_right = jnp.max(jnp.where(left, -jnp.inf, scores), 1, keepdims=True)
            expo = jnp.exp(scores - jnp.where(left, high_left, high_right))
            expo_ref[slot * pairs + pair] = expo.astype(BF16)
        return carry

    def weigh(slot, carry):
        for pair in range(pairs):
            expo = expo_ref[slot * pairs + pair]
            v = split(qkv_ref[rows_of(slot), pl.ds(2 * D + pair * 128, 128)])
            out_ref[rows_of(slot), pl.ds(pair * 128, 128)] = (
                matmul(expo, v) * (1.0 / matmul(expo, ones))
            ).astype(BF16)
        return carry

    for stage in (score, exponent, weigh):
        for slot in range(SLOTS):
            stage(slot, 0)


ATT_SCRATCH = [
    pltpu.VMEM((SLOTS * T, D), BF16),
    pltpu.VMEM((SLOTS * T, D), BF16),
    pltpu.VMEM((SLOTS * T, 3 * D), BF16),
    pltpu.VMEM((SLOTS * T, D), BF16),
    pltpu.VMEM((SLOTS * HEADS // 2, T, 128), F32),
    pltpu.VMEM((SLOTS * HEADS // 2, T, 128), BF16),
    pltpu.VMEM((D, 3 * D), BF16),
    pltpu.VMEM((D, D), BF16),
    pltpu.VMEM((D, 3 * D), BF16),
    pltpu.VMEM((D, D), BF16),
    pltpu.SemaphoreType.DMA((4,)),
]


def attend_kernel(
    me_ref,
    mine_ref,
    theirs_ref,
    local_ref,
    recv_ref,
    self_gain_ref,
    cross_gain_ref,
    mlp_gain_ref,
    self_qkv_hbm,
    self_out_hbm,
    cross_qkv_hbm,
    cross_out_hbm,
    after_ref,
    mlp_in_ref,
    x_ref,
    y_ref,
    qkv_ref,
    att_ref,
    score_ref,
    expo_ref,
    self_qkv,
    self_out,
    cross_qkv,
    cross_out,
    sems,
):
    side = me_ref[0] & 1
    copies = [
        pltpu.make_async_copy(src.at[side], dst, sems.at[n])
        for n, (src, dst) in enumerate(
            (
                (self_qkv_hbm, self_qkv),
                (self_out_hbm, self_out),
                (cross_qkv_hbm, cross_qkv),
                (cross_out_hbm, cross_out),
            )
        )
    ]
    for copy in copies:
        copy.start()

    def place(first_ref, second_ref):
        first_ref[0:64] = local_ref[4]
        first_ref[64:128] = jnp.where((mine_ref[2] & 1) == side, local_ref[2], recv_ref[3])
        first_ref[128:192] = recv_ref[4]
        first_ref[192:256] = jnp.where((theirs_ref[2] & 1) == side, local_ref[3], recv_ref[2])
        second_ref[0:64] = local_ref[0]
        second_ref[64:128] = local_ref[1]
        second_ref[128:192] = recv_ref[0]
        second_ref[192:256] = recv_ref[1]

    @pl.when(side == 0)
    def _():
        place(x_ref, y_ref)

    @pl.when(side == 1)
    def _():
        place(y_ref, x_ref)

    xn = normed(x_ref[...], self_gain_ref[pl.ds(side, 1), :])
    copies[0].wait()
    qkv_ref[...] = matmul(xn, self_qkv[...]).astype(BF16)
    attention(qkv_ref, score_ref, expo_ref, att_ref)
    copies[1].wait()
    after_self = (x_ref[...].astype(F32) + matmul(att_ref[...], self_out[...])).astype(BF16)
    x_ref[...] = after_self
    qn = normed(after_self, cross_gain_ref[pl.ds(2 * side, 1), :])
    yn = normed(y_ref[...], cross_gain_ref[pl.ds(2 * side + 1, 1), :])
    copies[2].wait()
    qkv_ref[:, 0:D] = matmul(qn, cross_qkv[:, 0:D]).astype(BF16)
    qkv_ref[:, D : 3 * D] = matmul(yn, cross_qkv[:, D : 3 * D]).astype(BF16)
    attention(qkv_ref, score_ref, expo_ref, att_ref)
    copies[3].wait()
    after_cross = (x_ref[...].astype(F32) + matmul(att_ref[...], cross_out[...])).astype(BF16)
    after_ref[...] = after_cross
    mlp_in_ref[...] = normed(after_cross, mlp_gain_ref[pl.ds(side, 1), :])


def gelu(v):
    return v * (lax.erf(v * 0.7071067811865476) + 1.0) * 0.5


def accumulate(count, mlp_in_ref, weights, acc_ref, held, sems):
    copies = [pltpu.make_async_copy(weights[n], held.at[n], sems.at[n]) for n in range(count)]
    for copy in copies:
        copy.start()
    for n in range(count):
        copies[n].wait()
        up = held[n, :, 0].reshape(384, D)
        down = held[n, :, 1].reshape(384, D)
        lifted = lax.dot_general(
            mlp_in_ref[...], up, (((1,), (1,)), ((), ())), preferred_element_type=F32
        )
        acc_ref[...] += matmul(gelu(lifted).astype(BF16), down)


def mlp_kernel(count, after_ref, mlp_in_ref, *refs):
    acc_ref, held, sems = refs[count:]
    acc_ref[...] = after_ref[...].astype(F32)
    accumulate(count, mlp_in_ref, refs[:count], acc_ref, held, sems)


def mlp_last_kernel(count, me_ref, mine_ref, theirs_ref, before_ref, mlp_in_ref, conf_ref, *refs):
    keep_ref, swap_ref, a_ref, b_ref, acc_ref, message, held, sems = refs[count:]
    acc_ref[...] = before_ref[...]
    accumulate(count, mlp_in_ref, refs[:count], acc_ref, held, sems)
    decoded = acc_ref[...].astype(BF16)
    conf = 1.0 + jnp.exp(jnp.sum(decoded.astype(F32) * conf_ref[...], -1, keepdims=True))
    high = conf.astype(BF16)
    rest = conf - high.astype(F32)
    middle = rest.astype(BF16)
    low = (rest - middle.astype(F32)).astype(BF16)
    lane = lax.broadcasted_iota(jnp.int32, (T, AUX), 1)
    side = me_ref[0] & 1
    for slot in range(SLOTS):
        rows = slice(slot * T, slot * T + T)
        ids = (mine_ref, theirs_ref)[slot // 2]
        held_by = jnp.where(side == 0, ids[2 * (slot % 2)], ids[2 * (slot % 2) + 1])
        owner = jnp.where(slot % 2 < ids[4], held_by, -1).astype(F32)
        aux = jnp.where(lane == 0, owner, 0.0)
        aux = jnp.where(lane == 1, high[rows].astype(F32), aux)
        aux = jnp.where(lane == 2, middle[rows].astype(F32), aux)
        aux = jnp.where(lane == 3, low[rows].astype(F32), aux)
        message[slot, :, 0:D] = decoded[rows]
        message[slot, :, D:MSG] = aux.astype(BF16)

    def put(ref, slots):
        for n, slot in enumerate(slots):
            ref[n] = message[slot]

    @pl.when(side == 0)
    def _():
        put(keep_ref, (0, 1, 3))
        put(swap_ref, (2, 1, 3))
        put(a_ref, (1, 3))
        put(b_ref, (1, 3))

    @pl.when(side == 1)
    def _():
        put(keep_ref, (0, 1, 1))
        put(swap_ref, (2, 3, 3))
        put(a_ref, (2, 3))
        put(b_ref, (0, 1))


def total_of(aux):
    return aux[:, 1:2] + aux[:, 2:3] + aux[:, 3:4]


def owner_of(ref, slot):
    lane = lax.broadcasted_iota(jnp.int32, (16, AUX), 1)
    aux = ref[slot, 0:16, D:MSG].astype(F32)
    return jnp.max(jnp.where(lane == 0, aux, -1.0)).astype(jnp.int32)


def add_to(sums, ref, slot):
    conf = total_of(ref[slot, :, D:MSG].astype(F32))
    sums[:, 0:D] += conf * ref[slot, :, 0:D].astype(F32)
    sums[:, D:MSG] += jnp.broadcast_to(conf, (T, AUX))


def load(core, when_0, when_1, held, sems):
    def copies(sources):
        at, made = 0, []
        for n, src in enumerate(sources):
            made.append(pltpu.make_async_copy(src, held.at[pl.ds(at, src.shape[0])], sems.at[n]))
            at += src.shape[0]
        return made

    @pl.when(core == 0)
    def _():
        for copy in copies(when_0):
            copy.start()

    @pl.when(core == 1)
    def _():
        for copy in copies(when_1):
            copy.start()

    return copies(when_0)


def middle_kernel(me_ref, keep, swapped, *refs):
    out_0 = refs[6]
    outs = refs[7:10]
    sums, held, sems = refs[10:]
    z, x, _, core = coordinates(me_ref[0])
    copies = load(
        core, [swapped.at[pl.ds(0, 2)], *refs[0:3]], [keep.at[pl.ds(0, 2)], *refs[3:6]], held, sems
    )
    sums[0:4] = jnp.zeros((4, T, MSG), F32)
    for n in range(8):
        if n % 2 == 0:
            copies[n // 2].wait()
        owner = owner_of(held, n)
        to_z, to_x, _, _ = coordinates(owner)
        here = jnp.where(core == 0, to_x == x, to_z == z)
        to = jnp.where(core == 0, to_z ^ z, to_x ^ x)
        add_to(sums.at[jnp.where((owner >= 0) & here, to, 4)], held, n)

    out_0[...] = sums[0]
    lane = lax.broadcasted_iota(jnp.int32, (T, AUX), 1)
    for mask, out in zip((1, 3, 2), outs):
        out[:, 0:D] = sums[mask, :, 0:D].astype(BF16)
        denominator = sums[mask, :, D:MSG]
        high = denominator.astype(BF16)
        rest = denominator - high.astype(F32)
        middle = rest.astype(BF16)
        low = rest - middle.astype(F32)
        aux = jnp.where(lane == 1, high.astype(F32), 0.0)
        aux = jnp.where(lane == 2, middle.astype(F32), aux)
        out[:, D:MSG] = jnp.where(lane == 3, low, aux).astype(BF16)


def row_kernel(me_ref, keep, swapped, *refs):
    sums, held, sems = refs[6:]
    me = me_ref[0]
    copies = load(me & 1, [keep, *refs[3:6]], [swapped, *refs[0:3]], held, sems)
    sums[...] = jnp.zeros((T, MSG), F32)
    for copy in copies:
        copy.wait()
    for n in range(9):

        @pl.when(owner_of(held, n) == me)
        def _(n=n):
            add_to(sums, held, n)


def final_kernel(column, row, from_1, from_3, from_2, head, out_ref):
    sums = column[...] + row[...]
    numerator, denominator = sums[:, 0:D], sums[:, D : D + 1]
    for piece in (from_1, from_3, from_2):
        numerator += piece[:, 0:D].astype(F32)
        denominator += total_of(piece[:, D:MSG].astype(F32))
    joined = (numerator / denominator).astype(BF16)
    out_ref[0] = matmul(joined, head[...]).astype(BF16)


def params(mib):
    return pltpu.CompilerParams(vmem_limit_bytes=mib * 2**20)


def shards(
    encoder_tokens,
    pair_list,
    pair_count,
    embed_weight,
    self_gain,
    self_qkv,
    self_out,
    cross_gain,
    cross_qkv,
    cross_out,
    mlp_gain,
    mlp_up,
    mlp_down,
    conf_weight,
    head_weight,
):
    me = lax.axis_index("row") * 8 + lax.axis_index("col")
    core = me & 1

    up_out, down_out = (lax.dynamic_index_in_dim(w, 1 - core, 0, False) for w in (mlp_up, mlp_down))
    came = swap(jnp.stack([up_out, down_out]))
    up_own, down_own = (lax.dynamic_index_in_dim(w, core, 0, False) for w in (mlp_up, mlp_down))
    mine = jnp.concatenate([pair_list.reshape(4), pair_count.reshape(1)])
    theirs = swap(mine)
    far = send(mine, ((Z, 1),), ((X, 1),))
    ids = (me.reshape(1), mine, theirs)

    own = jnp.einsum(
        "td,de->te", encoder_tokens[0], embed_weight, preferred_element_type=F32
    ).astype(BF16)

    block = jnp.concatenate([jnp.stack([up_own, down_own]), came], axis=1)
    block = join(block.reshape(96, D), own)[None]
    line = join(block, send(block, ((Y, 1),), ((Y, 3),)))
    line_far = send(line, ((Y, 3),), ((Y, 1),))

    def over_plane(held, first, last, one, two):
        near = send(held, ((first, 1),), ((first, 3),))
        held = join(held[:, :96], near[:, :96])
        held = join(held, send(held, ((first, 3),), ((first, 1),)))
        by_1 = send(held, ((last, one),), ((last, two),))
        by_3 = send(held, ((last, two),), ((last, one),))
        by_2 = send(by_1, ((last, two),), ((last, one),))
        return [h.reshape(8, 2, 48, D) for h in (held, by_1, by_3, by_2)]

    weights_a = over_plane(line, X, Z, 3, 1)
    weights_b = over_plane(line_far, Z, X, 1, 3)

    tokens = own[None]
    tokens = join(tokens, send(tokens, ((X, 1),), ((Z, 1),)))
    tokens = join(tokens, send(tokens, ((X, 3),), ((Z, 3),)))
    tokens = join(tokens, send(tokens, ((Z, 3),), ((X, 3),)))
    picked = pl.pallas_call(
        pick_kernel,
        out_shape=jax.ShapeDtypeStruct((2, T, D), BF16),
        in_specs=[SMEM] * 2 + [HBM],
        out_specs=VMEM,
        scratch_shapes=[pltpu.SemaphoreType.DMA((2,))],
        name="pick",
    )(ids[0], far, *in_hbm(tokens))
    tokens_far = send(picked, ((Z, 1),), ((X, 1),))
    selected = pl.pallas_call(
        select_kernel,
        out_shape=jax.ShapeDtypeStruct((5, T, D), BF16),
        in_specs=[SMEM] * 3 + [HBM] * 4 + [VMEM],
        out_specs=VMEM,
        scratch_shapes=[pltpu.SemaphoreType.DMA((4,))],
        name="select",
    )(*ids, *in_hbm(tokens, tokens_far, line, line_far), own)
    received = swap(selected)

    after, mlp_in = pl.pallas_call(
        attend_kernel,
        out_shape=[jax.ShapeDtypeStruct((SLOTS * T, D), BF16)] * 2,
        in_specs=[SMEM] * 3 + [VMEM] * 5 + [HBM] * 4,
        out_specs=[VMEM, VMEM],
        scratch_shapes=ATT_SCRATCH,
        compiler_params=params(32),
        name="attend",
    )(
        *ids,
        selected,
        received,
        self_gain,
        cross_gain.reshape(4, D),
        mlp_gain,
        *in_hbm(self_qkv, self_out, cross_qkv, cross_out),
    )

    def held_weights(count):
        return [pltpu.VMEM((count, 8, 2, 48, D), BF16), pltpu.SemaphoreType.DMA((count,))]

    sums = jax.ShapeDtypeStruct((SLOTS * T, D), F32)
    partial = pl.pallas_call(
        functools.partial(mlp_kernel, 6),
        out_shape=sums,
        in_specs=[VMEM] * 2 + [HBM] * 6,
        out_specs=VMEM,
        scratch_shapes=held_weights(6),
        compiler_params=params(32),
        name="lift",
    )(after, mlp_in, *weights_a[:3], *weights_b[:3])
    msg = lambda *shape: jax.ShapeDtypeStruct((*shape, MSG), BF16)
    keep, outgoing, piece_a, piece_b = pl.pallas_call(
        functools.partial(mlp_last_kernel, 2),
        out_shape=[msg(3, T), msg(3, T), msg(2, T), msg(2, T)],
        in_specs=[SMEM] * 3 + [VMEM] * 3 + [HBM] * 2,
        out_specs=[VMEM] * 4,
        scratch_shapes=[pltpu.VMEM((SLOTS * T, D), F32), pltpu.VMEM((SLOTS, T, MSG), BF16)]
        + held_weights(2),
        compiler_params=params(32),
        name="last",
    )(*ids, partial, mlp_in, conf_weight.reshape(1, D), weights_a[3], weights_b[3])

    incoming = swap(outgoing)
    masks = (1, 3, 2)
    got_a = [send(piece_a, ((Y, m), (C, 1)), ((X, m), (C, 1))) for m in masks]
    got_b = [send(piece_b, ((Y, m),), ((Z, m),)) for m in masks]
    pieces = in_hbm(keep, incoming, *got_a, *got_b)
    summed = jax.ShapeDtypeStruct((T, MSG), F32)
    column, *parts = pl.pallas_call(
        middle_kernel,
        out_shape=[summed] + [msg(T)] * 3,
        in_specs=[SMEM] + [HBM] * 8,
        out_specs=[VMEM] * 4,
        scratch_shapes=[
            pltpu.VMEM((5, T, MSG), F32),
            pltpu.VMEM((8, T, MSG), BF16),
            pltpu.SemaphoreType.DMA((4,)),
        ],
        name="middle",
    )(ids[0], *pieces)
    last = [send(s, ((Z, m),), ((X, m),)) for s, m in zip(parts, masks)]
    row = pl.pallas_call(
        row_kernel,
        out_shape=summed,
        in_specs=[SMEM] + [HBM] * 8,
        out_specs=VMEM,
        scratch_shapes=[pltpu.VMEM((9, T, MSG), BF16), pltpu.SemaphoreType.DMA((4,))],
        name="rows",
    )(ids[0], *pieces)
    return pl.pallas_call(
        final_kernel,
        out_shape=jax.ShapeDtypeStruct((1, T, 1024), BF16),
        in_specs=[VMEM] * 6,
        out_specs=VMEM,
        name="head",
    )(column, row, *last, head_weight)


def solution(mesh):
    return jax.shard_map(
        shards,
        mesh=mesh,
        in_specs=(
            P(("row", "col"), None, None),
            P("row", "col", None, None),
            P("row", "col"),
            P(),
            P(),
            P(),
            P(),
            P(),
            P(),
            P(),
            P(),
            P(None, ("row", "col"), None),
            P(None, ("row", "col"), None),
            P(),
            P(),
        ),
        out_specs=P(("row", "col"), None, None),
        check_vma=False,
    )
```

```python
import functools

import jax
import jax.numpy as jnp
from jax import lax
from jax.experimental import pallas as pl
from jax.experimental.pallas import tpu as pltpu
from jax.sharding import PartitionSpec as P


HEADS = 12
HEAD_DIM = 64
NORM_EPSILON = 1e-05
D = 768
T = 64
SLOTS = 4
AUX = 128
MSG = D + AUX
F32 = jnp.float32
BF16 = jnp.bfloat16
AXES = ("row", "col")


def coords(i):
    return i // 32, (i // 8) % 4, (i // 2) % 4, i % 2


def linear(z, x, y, c):
    return ((z * 4 + x) * 4 + y) * 2 + c


Z, X, Y, C = 0, 1, 2, 3


def send(array, core0, core1):
    pairs = []
    for i in range(128):
        at = list(coords(i))
        for dim, mask in (core0, core1)[at[3]]:
            at[dim] ^= mask
        pairs.append((i, linear(*at)))
    return lax.ppermute(array, AXES, pairs)


def swap(array):
    return send(array, ((C, 1),), ((C, 1),))


def join(*arrays):
    return jnp.concatenate(arrays, axis=0)


def place(delta, order):
    found = jnp.int32(0)
    for at, mask in enumerate(order):
        found = jnp.where(delta == mask, at, found)
    return found


def coordinates(me):
    return me >> 5, (me >> 3) & 3, (me >> 1) & 3, me & 1


VMEM = pl.BlockSpec(memory_space=pltpu.VMEM)
SMEM = pl.BlockSpec(memory_space=pltpu.SMEM)
HBM = pl.BlockSpec(memory_space=pltpu.HBM)


def in_hbm(*arrays):
    return [pltpu.with_memory_space_constraint(a, pltpu.HBM) for a in arrays]


def seconds_at(ids_ref, z, x, core):
    found = []
    for second in (ids_ref[1], ids_ref[3]):
        to_z, to_x, _, _ = coordinates(second)
        last = jnp.where(core == 0, z ^ to_z, x ^ to_x)
        first = jnp.where(core == 0, x ^ to_x, z ^ to_z)
        found.append((last, (last >> 1) * 4 + place(first, (0, 1, 3, 2))))
    return found


def pick_kernel(me_ref, far_ref, tokens, out_ref, sems):
    z, x, _, core = coordinates(me_ref[0])
    copies = [
        pltpu.make_async_copy(tokens.at[at], out_ref.at[n], sems.at[n])
        for n, (_, at) in enumerate(seconds_at(far_ref, z, x, core))
    ]
    for copy in copies:
        copy.start()
    for copy in copies:
        copy.wait()


def select_kernel(me_ref, mine_ref, theirs_ref, tokens, tokens_far, line, line_far, own, out_ref, sems):
    z, x, y, core = coordinates(me_ref[0])
    for n, (last, at) in enumerate(seconds_at(mine_ref, z, x, core)):

        @pl.when((last == 0) | (last == 3))
        def _(n=n, at=at):
            pltpu.make_async_copy(tokens.at[at], out_ref.at[n], sems.at[n]).start()

        @pl.when((last == 1) | (last == 2))
        def _(n=n):
            pltpu.make_async_copy(tokens_far.at[n], out_ref.at[n], sems.at[n]).start()

    for n, first in ((2, mine_ref[2]), (3, theirs_ref[2])):
        delta = y ^ ((first >> 1) & 3)
        at = jnp.where(core == 0, place(delta, (0, 1, 3, 2)), place(delta, (0, 3, 1, 2)))

        @pl.when(at < 2)
        def _(n=n, at=at):
            pltpu.make_async_copy(line.at[at, pl.ds(96, T)], out_ref.at[n], sems.at[n]).start()

        @pl.when(at >= 2)
        def _(n=n, at=at):
            pltpu.make_async_copy(line_far.at[at - 2, pl.ds(96, T)], out_ref.at[n], sems.at[n]).start()

    out_ref[4] = own[...]
    for n in range(4):
        pltpu.make_async_copy(own, out_ref.at[n], sems.at[n]).wait()


def normed(values, gain):
    values = values.astype(F32)
    centered = values - jnp.mean(values, -1, keepdims=True)
    variance = jnp.mean(centered * centered, -1, keepdims=True)
    return (centered * lax.rsqrt(variance + NORM_EPSILON) * gain).astype(BF16)


def matmul(a, b):
    return lax.dot_general(a, b, (((1,), (0,)), ((), ())), preferred_element_type=F32)


def attention(qkv_ref, score_ref, expo_ref, out_ref):
    pairs = HEADS // 2
    left = lax.broadcasted_iota(jnp.int32, (T, 128), 1) < HEAD_DIM
    same = (lax.broadcasted_iota(jnp.int32, (128, 128), 0) < HEAD_DIM) == (
        lax.broadcasted_iota(jnp.int32, (128, 128), 1) < HEAD_DIM
    )
    ones = jnp.where(same, 1.0, 0.0).astype(BF16)

    def rows_of(slot):
        return pl.ds(slot * T, T)

    def split(both):
        zero = jnp.zeros_like(both)
        return jnp.concatenate([jnp.where(left, both, zero), jnp.where(left, zero, both)], axis=0)

    def score(slot, carry):
        for pair in range(pairs):
            q = qkv_ref[rows_of(slot), pl.ds(pair * 128, 128)]
            k = split(qkv_ref[rows_of(slot), pl.ds(D + pair * 128, 128)])
            score_ref[slot * pairs + pair] = lax.dot_general(
                q, k, (((1,), (1,)), ((), ())), preferred_element_type=F32
            )
        return carry

    def exponent(slot, carry):
        for pair in range(pairs):
            scores = score_ref[slot * pairs + pair] * 0.125
            high_left = jnp.max(jnp.where(left, scores, -jnp.inf), 1, keepdims=True)
            high_right = jnp.max(jnp.where(left, -jnp.inf, scores), 1, keepdims=True)
            expo = jnp.exp(scores - jnp.where(left, high_left, high_right))
            expo_ref[slot * pairs + pair] = expo.astype(BF16)
        return carry

    def weigh(slot, carry):
        for pair in range(pairs):
            expo = expo_ref[slot * pairs + pair]
            v = split(qkv_ref[rows_of(slot), pl.ds(2 * D + pair * 128, 128)])
            out_ref[rows_of(slot), pl.ds(pair * 128, 128)] = (
                matmul(expo, v) * (1.0 / matmul(expo, ones))
            ).astype(BF16)
        return carry

    for stage in (score, exponent, weigh):
        for slot in range(SLOTS):
            stage(slot, 0)


ATT_SCRATCH = [
    pltpu.VMEM((SLOTS * T, D), BF16),
    pltpu.VMEM((SLOTS * T, D), BF16),
    pltpu.VMEM((SLOTS * T, 3 * D), BF16),
    pltpu.VMEM((SLOTS * T, D), BF16),
    pltpu.VMEM((SLOTS * HEADS // 2, T, 128), F32),
    pltpu.VMEM((SLOTS * HEADS // 2, T, 128), BF16),
    pltpu.VMEM((D, 3 * D), BF16),
    pltpu.VMEM((D, D), BF16),
    pltpu.VMEM((D, 3 * D), BF16),
    pltpu.VMEM((D, D), BF16),
    pltpu.SemaphoreType.DMA((4,)),
]


def attend_kernel(
    me_ref,
    mine_ref,
    theirs_ref,
    local_ref,
    recv_ref,
    self_gain_ref,
    cross_gain_ref,
    mlp_gain_ref,
    self_qkv_hbm,
    self_out_hbm,
    cross_qkv_hbm,
    cross_out_hbm,
    after_ref,
    mlp_in_ref,
    x_ref,
    y_ref,
    qkv_ref,
    att_ref,
    score_ref,
    expo_ref,
    self_qkv,
    self_out,
    cross_qkv,
    cross_out,
    sems,
):
    side = me_ref[0] & 1
    copies = [
        pltpu.make_async_copy(src.at[side], dst, sems.at[n])
        for n, (src, dst) in enumerate(
            (
                (self_qkv_hbm, self_qkv),
                (self_out_hbm, self_out),
                (cross_qkv_hbm, cross_qkv),
                (cross_out_hbm, cross_out),
            )
        )
    ]
    for copy in copies:
        copy.start()

    def place(first_ref, second_ref):
        first_ref[0:64] = local_ref[4]
        first_ref[64:128] = jnp.where((mine_ref[2] & 1) == side, local_ref[2], recv_ref[3])
        first_ref[128:192] = recv_ref[4]
        first_ref[192:256] = jnp.where((theirs_ref[2] & 1) == side, local_ref[3], recv_ref[2])
        second_ref[0:64] = local_ref[0]
        second_ref[64:128] = local_ref[1]
        second_ref[128:192] = recv_ref[0]
        second_ref[192:256] = recv_ref[1]

    @pl.when(side == 0)
    def _():
        place(x_ref, y_ref)

    @pl.when(side == 1)
    def _():
        place(y_ref, x_ref)

    xn = normed(x_ref[...], self_gain_ref[pl.ds(side, 1), :])
    copies[0].wait()
    qkv_ref[...] = matmul(xn, self_qkv[...]).astype(BF16)
    attention(qkv_ref, score_ref, expo_ref, att_ref)
    copies[1].wait()
    after_self = (x_ref[...].astype(F32) + matmul(att_ref[...], self_out[...])).astype(BF16)
    x_ref[...] = after_self
    qn = normed(after_self, cross_gain_ref[pl.ds(2 * side, 1), :])
    yn = normed(y_ref[...], cross_gain_ref[pl.ds(2 * side + 1, 1), :])
    copies[2].wait()
    qkv_ref[:, 0:D] = matmul(qn, cross_qkv[:, 0:D]).astype(BF16)
    qkv_ref[:, D : 3 * D] = matmul(yn, cross_qkv[:, D : 3 * D]).astype(BF16)
    attention(qkv_ref, score_ref, expo_ref, att_ref)
    copies[3].wait()
    after_cross = (x_ref[...].astype(F32) + matmul(att_ref[...], cross_out[...])).astype(BF16)
    after_ref[...] = after_cross
    mlp_in_ref[...] = normed(after_cross, mlp_gain_ref[pl.ds(side, 1), :])


def gelu(v):
    return v * (lax.erf(v * 0.7071067811865476) + 1.0) * 0.5


def accumulate(groups, mlp_in_ref, weights, acc_ref, held, sems):
    copies, at = [], 0
    for n, size in enumerate(groups):
        blocks = []
        for m in range(size):
            part = slice(m * 8 // size, (m + 1) * 8 // size)
            to = held.at[n, pl.ds(part.start, part.stop - part.start)]
            blocks.append(pltpu.make_async_copy(weights[at], to, sems.at[at]))
            at += 1
        copies.append(blocks)
    for blocks in copies:
        for copy in blocks:
            copy.start()
    for n, blocks in enumerate(copies):
        for copy in blocks:
            copy.wait()
        up = held[n, :, 0].reshape(384, D)
        down = held[n, :, 1].reshape(384, D)
        lifted = lax.dot_general(
            mlp_in_ref[...], up, (((1,), (1,)), ((), ())), preferred_element_type=F32
        )
        acc_ref[...] += matmul(gelu(lifted).astype(BF16), down)


def mlp_kernel(groups, after_ref, mlp_in_ref, *refs):
    count = sum(groups)
    acc_ref, held, sems = refs[count:]
    acc_ref[...] = after_ref[...].astype(F32)
    accumulate(groups, mlp_in_ref, refs[:count], acc_ref, held, sems)


def mlp_last_kernel(groups, me_ref, mine_ref, theirs_ref, before_ref, mlp_in_ref, conf_ref, *refs):
    count = sum(groups)
    keep_ref, swap_ref, a_ref, b_ref, acc_ref, message, held, sems = refs[count:]
    acc_ref[...] = before_ref[...]
    accumulate(groups, mlp_in_ref, refs[:count], acc_ref, held, sems)
    decoded = acc_ref[...].astype(BF16)
    conf = 1.0 + jnp.exp(jnp.sum(decoded.astype(F32) * conf_ref[...], -1, keepdims=True))
    high = conf.astype(BF16)
    rest = conf - high.astype(F32)
    middle = rest.astype(BF16)
    low = (rest - middle.astype(F32)).astype(BF16)
    lane = lax.broadcasted_iota(jnp.int32, (T, AUX), 1)
    side = me_ref[0] & 1
    for slot in range(SLOTS):
        rows = slice(slot * T, slot * T + T)
        ids = (mine_ref, theirs_ref)[slot // 2]
        held_by = jnp.where(side == 0, ids[2 * (slot % 2)], ids[2 * (slot % 2) + 1])
        owner = jnp.where(slot % 2 < ids[4], held_by, -1).astype(F32)
        aux = jnp.where(lane == 0, owner, 0.0)
        aux = jnp.where(lane == 1, high[rows].astype(F32), aux)
        aux = jnp.where(lane == 2, middle[rows].astype(F32), aux)
        aux = jnp.where(lane == 3, low[rows].astype(F32), aux)
        message[slot, :, 0:D] = decoded[rows]
        message[slot, :, D:MSG] = aux.astype(BF16)

    def put(ref, slots):
        for n, slot in enumerate(slots):
            ref[n] = message[slot]

    @pl.when(side == 0)
    def _():
        put(keep_ref, (0, 1, 3))
        put(swap_ref, (2, 1, 3))
        put(a_ref, (1, 3))
        put(b_ref, (1, 3))

    @pl.when(side == 1)
    def _():
        put(keep_ref, (0, 1, 1))
        put(swap_ref, (2, 3, 3))
        put(a_ref, (2, 3))
        put(b_ref, (0, 1))


def total_of(aux):
    return aux[:, 1:2] + aux[:, 2:3] + aux[:, 3:4]


def owner_of(ref, slot):
    lane = lax.broadcasted_iota(jnp.int32, (16, AUX), 1)
    aux = ref[slot, 0:16, D:MSG].astype(F32)
    return jnp.max(jnp.where(lane == 0, aux, -1.0)).astype(jnp.int32)


def add_to(sums, ref, slot):
    conf = total_of(ref[slot, :, D:MSG].astype(F32))
    sums[:, 0:D] += conf * ref[slot, :, 0:D].astype(F32)
    sums[:, D:MSG] += jnp.broadcast_to(conf, (T, AUX))


def load(core, when_0, when_1, held, sems):
    def copies(sources):
        at, made = 0, []
        for n, src in enumerate(sources):
            made.append(pltpu.make_async_copy(src, held.at[pl.ds(at, src.shape[0])], sems.at[n]))
            at += src.shape[0]
        return made

    @pl.when(core == 0)
    def _():
        for copy in copies(when_0):
            copy.start()

    @pl.when(core == 1)
    def _():
        for copy in copies(when_1):
            copy.start()

    return copies(when_0)


def middle_kernel(me_ref, keep, swapped, *refs):
    out_0 = refs[6]
    outs = refs[7:10]
    sums, held, sems = refs[10:]
    z, x, _, core = coordinates(me_ref[0])
    copies = load(
        core, [swapped.at[pl.ds(0, 2)], *refs[0:3]], [keep.at[pl.ds(0, 2)], *refs[3:6]], held, sems
    )
    sums[0:4] = jnp.zeros((4, T, MSG), F32)
    for n in range(8):
        if n % 2 == 0:
            copies[n // 2].wait()
        owner = owner_of(held, n)
        to_z, to_x, _, _ = coordinates(owner)
        here = jnp.where(core == 0, to_x == x, to_z == z)
        to = jnp.where(core == 0, to_z ^ z, to_x ^ x)
        add_to(sums.at[jnp.where((owner >= 0) & here, to, 4)], held, n)

    out_0[...] = sums[0]
    lane = lax.broadcasted_iota(jnp.int32, (T, AUX), 1)
    for mask, out in zip((1, 3, 2), outs):
        out[:, 0:D] = sums[mask, :, 0:D].astype(BF16)
        denominator = sums[mask, :, D:MSG]
        high = denominator.astype(BF16)
        rest = denominator - high.astype(F32)
        middle = rest.astype(BF16)
        low = rest - middle.astype(F32)
        aux = jnp.where(lane == 1, high.astype(F32), 0.0)
        aux = jnp.where(lane == 2, middle.astype(F32), aux)
        out[:, D:MSG] = jnp.where(lane == 3, low, aux).astype(BF16)


def row_kernel(me_ref, keep, swapped, *refs):
    sums, held, sems = refs[6:]
    me = me_ref[0]
    copies = load(me & 1, [keep, *refs[3:6]], [swapped, *refs[0:3]], held, sems)
    sums[...] = jnp.zeros((T, MSG), F32)
    for copy in copies:
        copy.wait()
    for n in range(9):

        @pl.when(owner_of(held, n) == me)
        def _(n=n):
            add_to(sums, held, n)


def final_kernel(column, row, from_1, from_3, from_2, head, out_ref):
    sums = column[...] + row[...]
    numerator, denominator = sums[:, 0:D], sums[:, D : D + 1]
    for piece in (from_1, from_3, from_2):
        numerator += piece[:, 0:D].astype(F32)
        denominator += total_of(piece[:, D:MSG].astype(F32))
    joined = (numerator / denominator).astype(BF16)
    out_ref[0] = matmul(joined, head[...]).astype(BF16)


def params(mib):
    return pltpu.CompilerParams(vmem_limit_bytes=mib * 2**20)


def shards(
    encoder_tokens,
    pair_list,
    pair_count,
    embed_weight,
    self_gain,
    self_qkv,
    self_out,
    cross_gain,
    cross_qkv,
    cross_out,
    mlp_gain,
    mlp_up,
    mlp_down,
    conf_weight,
    head_weight,
):
    me = lax.axis_index("row") * 8 + lax.axis_index("col")
    core = me & 1

    up_out, down_out = (lax.dynamic_index_in_dim(w, 1 - core, 0, False) for w in (mlp_up, mlp_down))
    came = swap(jnp.stack([up_out, down_out]))
    up_own, down_own = (lax.dynamic_index_in_dim(w, core, 0, False) for w in (mlp_up, mlp_down))
    mine = jnp.concatenate([pair_list.reshape(4), pair_count.reshape(1)])
    theirs = swap(mine)
    far = send(mine, ((Z, 1),), ((X, 1),))
    ids = (me.reshape(1), mine, theirs)

    own = jnp.einsum(
        "td,de->te", encoder_tokens[0], embed_weight, preferred_element_type=F32
    ).astype(BF16)

    block = jnp.concatenate([jnp.stack([up_own, down_own]), came], axis=1)
    block = join(block.reshape(96, D), own)[None]
    line = join(block, send(block, ((Y, 1),), ((Y, 3),)))
    line_far = send(line, ((Y, 3),), ((Y, 1),))

    def over_plane(held, first, last, one, two):
        near = send(held, ((first, 1),), ((first, 3),))
        held = join(held[:, :96], near[:, :96])
        held = join(held, send(held, ((first, 3),), ((first, 1),)))
        near = send(held, ((last, one),), ((last, two),))
        half = lax.dynamic_slice_in_dim(held, ((me >> 1) & 1) * 4, 4, 0)
        far = send(half, ((last, two),), ((last, one),))
        rest = send(far, ((Y, 1),), ((Y, 3),))
        across = send(near, ((last, two),), ((last, one),))
        return [h.reshape(-1, 2, 48, D) for h in (held, near, far, rest, across)]

    weights_a = over_plane(line, X, Z, 3, 1)
    weights_b = over_plane(line_far, Z, X, 1, 3)

    tokens = own[None]
    tokens = join(tokens, send(tokens, ((X, 1),), ((Z, 1),)))
    tokens = join(tokens, send(tokens, ((X, 3),), ((Z, 3),)))
    tokens = join(tokens, send(tokens, ((Z, 3),), ((X, 3),)))
    picked = pl.pallas_call(
        pick_kernel,
        out_shape=jax.ShapeDtypeStruct((2, T, D), BF16),
        in_specs=[SMEM] * 2 + [HBM],
        out_specs=VMEM,
        scratch_shapes=[pltpu.SemaphoreType.DMA((2,))],
        name="pick",
    )(ids[0], far, *in_hbm(tokens))
    tokens_far = send(picked, ((Z, 1),), ((X, 1),))
    selected = pl.pallas_call(
        select_kernel,
        out_shape=jax.ShapeDtypeStruct((5, T, D), BF16),
        in_specs=[SMEM] * 3 + [HBM] * 4 + [VMEM],
        out_specs=VMEM,
        scratch_shapes=[pltpu.SemaphoreType.DMA((4,))],
        name="select",
    )(*ids, *in_hbm(tokens, tokens_far, line, line_far), own)
    received = swap(selected)

    after, mlp_in = pl.pallas_call(
        attend_kernel,
        out_shape=[jax.ShapeDtypeStruct((SLOTS * T, D), BF16)] * 2,
        in_specs=[SMEM] * 3 + [VMEM] * 5 + [HBM] * 4,
        out_specs=[VMEM, VMEM],
        scratch_shapes=ATT_SCRATCH,
        compiler_params=params(32),
        name="attend",
    )(
        *ids,
        selected,
        received,
        self_gain,
        cross_gain.reshape(4, D),
        mlp_gain,
        *in_hbm(self_qkv, self_out, cross_qkv, cross_out),
    )

    def held_weights(groups):
        return [pltpu.VMEM((len(groups), 8, 2, 48, D), BF16), pltpu.SemaphoreType.DMA((sum(groups),))]

    early, late = (1, 1, 1, 1, 2), (2, 1, 1)

    sums = jax.ShapeDtypeStruct((SLOTS * T, D), F32)
    partial = pl.pallas_call(
        functools.partial(mlp_kernel, early),
        out_shape=sums,
        in_specs=[VMEM] * 2 + [HBM] * sum(early),
        out_specs=VMEM,
        scratch_shapes=held_weights(early),
        compiler_params=params(32),
        name="lift",
    )(
        after,
        mlp_in,
        *(weights_a[0], weights_b[0], weights_a[1], weights_b[1], weights_a[2], weights_a[3]),
    )
    msg = lambda *shape: jax.ShapeDtypeStruct((*shape, MSG), BF16)
    keep, outgoing, piece_a, piece_b = pl.pallas_call(
        functools.partial(mlp_last_kernel, late),
        out_shape=[msg(3, T), msg(3, T), msg(2, T), msg(2, T)],
        in_specs=[SMEM] * 3 + [VMEM] * 3 + [HBM] * sum(late),
        out_specs=[VMEM] * 4,
        scratch_shapes=[pltpu.VMEM((SLOTS * T, D), F32), pltpu.VMEM((SLOTS, T, MSG), BF16)]
        + held_weights(late),
        compiler_params=params(32),
        name="last",
    )(
        *ids,
        partial,
        mlp_in,
        conf_weight.reshape(1, D),
        *(weights_b[2], weights_b[3], weights_a[4], weights_b[4]),
    )

    incoming = swap(outgoing)
    masks = (1, 3, 2)
    got_a = [send(piece_a, ((Y, m), (C, 1)), ((X, m), (C, 1))) for m in masks]
    got_b = [send(piece_b, ((Y, m),), ((Z, m),)) for m in masks]
    pieces = in_hbm(keep, incoming, *got_a, *got_b)
    summed = jax.ShapeDtypeStruct((T, MSG), F32)
    column, *parts = pl.pallas_call(
        middle_kernel,
        out_shape=[summed] + [msg(T)] * 3,
        in_specs=[SMEM] + [HBM] * 8,
        out_specs=[VMEM] * 4,
        scratch_shapes=[
            pltpu.VMEM((5, T, MSG), F32),
            pltpu.VMEM((8, T, MSG), BF16),
            pltpu.SemaphoreType.DMA((4,)),
        ],
        name="middle",
    )(ids[0], *pieces)
    last = [send(s, ((Z, m),), ((X, m),)) for s, m in zip(parts, masks)]
    row = pl.pallas_call(
        row_kernel,
        out_shape=summed,
        in_specs=[SMEM] + [HBM] * 8,
        out_specs=VMEM,
        scratch_shapes=[pltpu.VMEM((9, T, MSG), BF16), pltpu.SemaphoreType.DMA((4,))],
        name="rows",
    )(ids[0], *pieces)
    return pl.pallas_call(
        final_kernel,
        out_shape=jax.ShapeDtypeStruct((1, T, 1024), BF16),
        in_specs=[VMEM] * 6,
        out_specs=VMEM,
        name="head",
    )(column, row, *last, head_weight)


def solution(mesh):
    return jax.shard_map(
        shards,
        mesh=mesh,
        in_specs=(
            P(("row", "col"), None, None),
            P("row", "col", None, None),
            P("row", "col"),
            P(),
            P(),
            P(),
            P(),
            P(),
            P(),
            P(),
            P(),
            P(None, ("row", "col"), None),
            P(None, ("row", "col"), None),
            P(),
            P(),
        ),
        out_specs=P(("row", "col"), None, None),
        check_vma=False,
    )
```

```python
import functools

import jax
import jax.numpy as jnp
from jax import lax
from jax.experimental import pallas as pl
from jax.experimental.pallas import tpu as pltpu
from jax.sharding import PartitionSpec as P


HEADS = 12
HEAD_DIM = 64
NORM_EPSILON = 1e-05
D = 768
T = 64
SLOTS = 4
AUX = 128
MSG = D + AUX
F32 = jnp.float32
BF16 = jnp.bfloat16
AXES = ("row", "col")


def coords(i):
    return i // 32, (i // 8) % 4, (i // 2) % 4, i % 2


def linear(z, x, y, c):
    return ((z * 4 + x) * 4 + y) * 2 + c


Z, X, Y, C = 0, 1, 2, 3


def send(array, core0, core1):
    pairs = []
    for i in range(128):
        at = list(coords(i))
        for dim, mask in (core0, core1)[at[3]]:
            at[dim] ^= mask
        pairs.append((i, linear(*at)))
    return lax.ppermute(array, AXES, pairs)


def swap(array):
    return send(array, ((C, 1),), ((C, 1),))


def join(*arrays):
    return jnp.concatenate(arrays, axis=0)


def place(delta, order):
    found = jnp.int32(0)
    for at, mask in enumerate(order):
        found = jnp.where(delta == mask, at, found)
    return found


def coordinates(me):
    return me >> 5, (me >> 3) & 3, (me >> 1) & 3, me & 1


VMEM = pl.BlockSpec(memory_space=pltpu.VMEM)
SMEM = pl.BlockSpec(memory_space=pltpu.SMEM)
HBM = pl.BlockSpec(memory_space=pltpu.HBM)


def in_hbm(*arrays):
    return [pltpu.with_memory_space_constraint(a, pltpu.HBM) for a in arrays]


def seconds_at(ids_ref, z, x, core):
    found = []
    for second in (ids_ref[1], ids_ref[3]):
        to_z, to_x, _, _ = coordinates(second)
        last = jnp.where(core == 0, z ^ to_z, x ^ to_x)
        first = jnp.where(core == 0, x ^ to_x, z ^ to_z)
        found.append((last, (last >> 1) * 4 + place(first, (0, 1, 3, 2))))
    return found


def pick_kernel(me_ref, far_ref, tokens, out_ref, sems):
    z, x, _, core = coordinates(me_ref[0])
    copies = [
        pltpu.make_async_copy(tokens.at[at], out_ref.at[n], sems.at[n])
        for n, (_, at) in enumerate(seconds_at(far_ref, z, x, core))
    ]
    for copy in copies:
        copy.start()
    for copy in copies:
        copy.wait()


def select_kernel(me_ref, mine_ref, theirs_ref, tokens, tokens_far, line, line_far, own, out_ref, sems):
    z, x, y, core = coordinates(me_ref[0])
    for n, (last, at) in enumerate(seconds_at(mine_ref, z, x, core)):

        @pl.when((last == 0) | (last == 3))
        def _(n=n, at=at):
            pltpu.make_async_copy(tokens.at[at], out_ref.at[n], sems.at[n]).start()

        @pl.when((last == 1) | (last == 2))
        def _(n=n):
            pltpu.make_async_copy(tokens_far.at[n], out_ref.at[n], sems.at[n]).start()

    for n, first in ((2, mine_ref[2]), (3, theirs_ref[2])):
        delta = y ^ ((first >> 1) & 3)
        at = jnp.where(core == 0, place(delta, (0, 1, 3, 2)), place(delta, (0, 3, 1, 2)))

        @pl.when(at < 2)
        def _(n=n, at=at):
            pltpu.make_async_copy(line.at[at, pl.ds(96, T)], out_ref.at[n], sems.at[n]).start()

        @pl.when(at >= 2)
        def _(n=n, at=at):
            pltpu.make_async_copy(line_far.at[at - 2, pl.ds(96, T)], out_ref.at[n], sems.at[n]).start()

    out_ref[4] = own[...]
    for n in range(4):
        pltpu.make_async_copy(own, out_ref.at[n], sems.at[n]).wait()


def normed(values, gain):
    values = values.astype(F32)
    centered = values - jnp.mean(values, -1, keepdims=True)
    variance = jnp.mean(centered * centered, -1, keepdims=True)
    return (centered * lax.rsqrt(variance + NORM_EPSILON) * gain).astype(BF16)


def matmul(a, b):
    return lax.dot_general(a, b, (((1,), (0,)), ((), ())), preferred_element_type=F32)


def attention(qkv_ref, score_ref, expo_ref, out_ref):
    pairs = HEADS // 2
    left = lax.broadcasted_iota(jnp.int32, (T, 128), 1) < HEAD_DIM
    same = (lax.broadcasted_iota(jnp.int32, (128, 128), 0) < HEAD_DIM) == (
        lax.broadcasted_iota(jnp.int32, (128, 128), 1) < HEAD_DIM
    )
    ones = jnp.where(same, 1.0, 0.0).astype(BF16)

    def rows_of(slot):
        return pl.ds(slot * T, T)

    def split(both):
        zero = jnp.zeros_like(both)
        return jnp.concatenate([jnp.where(left, both, zero), jnp.where(left, zero, both)], axis=0)

    def score(slot, carry):
        for pair in range(pairs):
            q = qkv_ref[rows_of(slot), pl.ds(pair * 128, 128)]
            k = split(qkv_ref[rows_of(slot), pl.ds(D + pair * 128, 128)])
            score_ref[slot * pairs + pair] = lax.dot_general(
                q, k, (((1,), (1,)), ((), ())), preferred_element_type=F32
            )
        return carry

    def exponent(slot, carry):
        for pair in range(pairs):
            scores = score_ref[slot * pairs + pair] * 0.125
            high_left = jnp.max(jnp.where(left, scores, -jnp.inf), 1, keepdims=True)
            high_right = jnp.max(jnp.where(left, -jnp.inf, scores), 1, keepdims=True)
            expo = jnp.exp(scores - jnp.where(left, high_left, high_right))
            expo_ref[slot * pairs + pair] = expo.astype(BF16)
        return carry

    def weigh(slot, carry):
        for pair in range(pairs):
            expo = expo_ref[slot * pairs + pair]
            v = split(qkv_ref[rows_of(slot), pl.ds(2 * D + pair * 128, 128)])
            out_ref[rows_of(slot), pl.ds(pair * 128, 128)] = (
                matmul(expo, v) * (1.0 / matmul(expo, ones))
            ).astype(BF16)
        return carry

    for stage in (score, exponent, weigh):
        for slot in range(SLOTS):
            stage(slot, 0)


ATT_SCRATCH = [
    pltpu.VMEM((SLOTS * T, D), BF16),
    pltpu.VMEM((SLOTS * T, D), BF16),
    pltpu.VMEM((SLOTS * T, 3 * D), BF16),
    pltpu.VMEM((SLOTS * T, D), BF16),
    pltpu.VMEM((SLOTS * HEADS // 2, T, 128), F32),
    pltpu.VMEM((SLOTS * HEADS // 2, T, 128), BF16),
    pltpu.VMEM((D, 3 * D), BF16),
    pltpu.VMEM((D, D), BF16),
    pltpu.VMEM((D, 3 * D), BF16),
    pltpu.VMEM((D, D), BF16),
    pltpu.SemaphoreType.DMA((4,)),
]


def attend_kernel(
    me_ref,
    mine_ref,
    theirs_ref,
    local_ref,
    recv_ref,
    self_gain_ref,
    cross_gain_ref,
    mlp_gain_ref,
    self_qkv_hbm,
    self_out_hbm,
    cross_qkv_hbm,
    cross_out_hbm,
    after_ref,
    mlp_in_ref,
    x_ref,
    y_ref,
    qkv_ref,
    att_ref,
    score_ref,
    expo_ref,
    self_qkv,
    self_out,
    cross_qkv,
    cross_out,
    sems,
):
    side = me_ref[0] & 1
    copies = [
        pltpu.make_async_copy(src.at[side], dst, sems.at[n])
        for n, (src, dst) in enumerate(
            (
                (self_qkv_hbm, self_qkv),
                (self_out_hbm, self_out),
                (cross_qkv_hbm, cross_qkv),
                (cross_out_hbm, cross_out),
            )
        )
    ]
    for copy in copies:
        copy.start()

    def place(first_ref, second_ref):
        first_ref[0:64] = local_ref[4]
        first_ref[64:128] = jnp.where((mine_ref[2] & 1) == side, local_ref[2], recv_ref[3])
        first_ref[128:192] = recv_ref[4]
        first_ref[192:256] = jnp.where((theirs_ref[2] & 1) == side, local_ref[3], recv_ref[2])
        second_ref[0:64] = local_ref[0]
        second_ref[64:128] = local_ref[1]
        second_ref[128:192] = recv_ref[0]
        second_ref[192:256] = recv_ref[1]

    @pl.when(side == 0)
    def _():
        place(x_ref, y_ref)

    @pl.when(side == 1)
    def _():
        place(y_ref, x_ref)

    xn = normed(x_ref[...], self_gain_ref[pl.ds(side, 1), :])
    copies[0].wait()
    qkv_ref[...] = matmul(xn, self_qkv[...]).astype(BF16)
    attention(qkv_ref, score_ref, expo_ref, att_ref)
    copies[1].wait()
    after_self = (x_ref[...].astype(F32) + matmul(att_ref[...], self_out[...])).astype(BF16)
    x_ref[...] = after_self
    qn = normed(after_self, cross_gain_ref[pl.ds(2 * side, 1), :])
    yn = normed(y_ref[...], cross_gain_ref[pl.ds(2 * side + 1, 1), :])
    copies[2].wait()
    qkv_ref[:, 0:D] = matmul(qn, cross_qkv[:, 0:D]).astype(BF16)
    qkv_ref[:, D : 3 * D] = matmul(yn, cross_qkv[:, D : 3 * D]).astype(BF16)
    attention(qkv_ref, score_ref, expo_ref, att_ref)
    copies[3].wait()
    after_cross = (x_ref[...].astype(F32) + matmul(att_ref[...], cross_out[...])).astype(BF16)
    after_ref[...] = after_cross
    mlp_in_ref[...] = normed(after_cross, mlp_gain_ref[pl.ds(side, 1), :])


def gelu(v):
    return v * (lax.erf(v * 0.7071067811865476) + 1.0) * 0.5


def accumulate(groups, mlp_in_ref, weights, acc_ref, held, sems):
    copies, at = [], 0
    for n, size in enumerate(groups):
        blocks = []
        for m in range(size):
            part = slice(m * 8 // size, (m + 1) * 8 // size)
            to = held.at[n, pl.ds(part.start, part.stop - part.start)]
            blocks.append(pltpu.make_async_copy(weights[at], to, sems.at[at]))
            at += 1
        copies.append(blocks)
    for blocks in copies:
        for copy in blocks:
            copy.start()
    for n, blocks in enumerate(copies):
        for copy in blocks:
            copy.wait()
        up = held[n, :, 0].reshape(384, D)
        down = held[n, :, 1].reshape(384, D)
        lifted = lax.dot_general(
            mlp_in_ref[...], up, (((1,), (1,)), ((), ())), preferred_element_type=F32
        )
        acc_ref[...] += matmul(gelu(lifted).astype(BF16), down)


def mlp_kernel(groups, after_ref, mlp_in_ref, *refs):
    count = sum(groups)
    acc_ref, held, sems = refs[count:]
    acc_ref[...] = after_ref[...].astype(F32)
    accumulate(groups, mlp_in_ref, refs[:count], acc_ref, held, sems)


def mlp_last_kernel(groups, me_ref, mine_ref, theirs_ref, before_ref, mlp_in_ref, conf_ref, *refs):
    count = sum(groups)
    own_ref, a_ref, b_ref, acc_ref, message, held, sems = refs[count:]
    acc_ref[...] = before_ref[...]
    accumulate(groups, mlp_in_ref, refs[:count], acc_ref, held, sems)
    decoded = acc_ref[...].astype(BF16)
    conf = 1.0 + jnp.exp(jnp.sum(decoded.astype(F32) * conf_ref[...], -1, keepdims=True))
    high = conf.astype(BF16)
    rest = conf - high.astype(F32)
    middle = rest.astype(BF16)
    low = (rest - middle.astype(F32)).astype(BF16)
    lane = lax.broadcasted_iota(jnp.int32, (T, AUX), 1)
    side = me_ref[0] & 1
    for slot in range(SLOTS):
        rows = slice(slot * T, slot * T + T)
        ids = (mine_ref, theirs_ref)[slot // 2]
        held_by = jnp.where(side == 0, ids[2 * (slot % 2)], ids[2 * (slot % 2) + 1])
        owner = jnp.where(slot % 2 < ids[4], held_by, -1).astype(F32)
        aux = jnp.where(lane == 0, owner, 0.0)
        aux = jnp.where(lane == 1, high[rows].astype(F32), aux)
        aux = jnp.where(lane == 2, middle[rows].astype(F32), aux)
        aux = jnp.where(lane == 3, low[rows].astype(F32), aux)
        message[slot, :, 0:D] = decoded[rows]
        message[slot, :, D:MSG] = aux.astype(BF16)

    def put(ref, slots):
        for n, slot in enumerate(slots):
            ref[n] = message[slot]

    @pl.when(side == 0)
    def _():
        put(own_ref, (0, 2))
        put(a_ref, (1, 3))
        put(b_ref, (1, 3))

    @pl.when(side == 1)
    def _():
        put(own_ref, (0, 2))
        put(a_ref, (2, 3))
        put(b_ref, (0, 1))


def total_of(aux):
    return aux[:, 1:2] + aux[:, 2:3] + aux[:, 3:4]


def owner_of(ref, slot):
    lane = lax.broadcasted_iota(jnp.int32, (16, AUX), 1)
    aux = ref[slot, 0:16, D:MSG].astype(F32)
    return jnp.max(jnp.where(lane == 0, aux, -1.0)).astype(jnp.int32)


def add_to(sums, ref, slot):
    conf = total_of(ref[slot, :, D:MSG].astype(F32))
    sums[:, 0:D] += conf * ref[slot, :, 0:D].astype(F32)
    sums[:, D:MSG] += jnp.broadcast_to(conf, (T, AUX))


def load(sources, held, sems):
    copies = [
        pltpu.make_async_copy(src, held.at[pl.ds(2 * n, 2)], sems.at[n]) for n, src in enumerate(sources)
    ]
    for copy in copies:
        copy.start()
    return copies


def middle_kernel(me_ref, *refs):
    out_0 = refs[8]
    outs = refs[9:12]
    sums, held, sems = refs[12:]
    z, x, _, core = coordinates(me_ref[0])

    @pl.when(core == 0)
    def _():
        load(refs[0:4], held, sems)

    @pl.when(core == 1)
    def _():
        load(refs[4:8], held, sems)

    copies = [pltpu.make_async_copy(refs[n], held.at[pl.ds(2 * n, 2)], sems.at[n]) for n in range(4)]
    sums[0:4] = jnp.zeros((4, T, MSG), F32)
    for n in range(8):
        if n % 2 == 0:
            copies[n // 2].wait()
        owner = owner_of(held, n)
        to_z, to_x, _, _ = coordinates(owner)
        here = jnp.where(core == 0, to_x == x, to_z == z)
        to = jnp.where(core == 0, to_z ^ z, to_x ^ x)
        add_to(sums.at[jnp.where((owner >= 0) & here, to, 4)], held, n)

    out_0[...] = sums[0]
    lane = lax.broadcasted_iota(jnp.int32, (T, AUX), 1)
    for mask, out in zip((1, 3, 2), outs):
        out[:, 0:D] = sums[mask, :, 0:D].astype(BF16)
        denominator = sums[mask, :, D:MSG]
        high = denominator.astype(BF16)
        rest = denominator - high.astype(F32)
        middle = rest.astype(BF16)
        low = rest - middle.astype(F32)
        aux = jnp.where(lane == 1, high.astype(F32), 0.0)
        aux = jnp.where(lane == 2, middle.astype(F32), aux)
        out[:, D:MSG] = jnp.where(lane == 3, low, aux).astype(BF16)


def row_kernel(me_ref, *refs):
    mine, theirs, held, sems = refs[5:]
    me = me_ref[0]
    mine[...] = jnp.zeros((T, MSG), F32)
    theirs[...] = jnp.zeros((T, MSG), F32)

    @pl.when((me & 1) == 0)
    def _():
        copies = load(refs[:5], held, sems)
        for n in range(10):
            if n % 2 == 0:
                copies[n // 2].wait()
            owner = owner_of(held, n)

            @pl.when(owner == me)
            def _(n=n):
                add_to(mine, held, n)

            @pl.when(owner == me + 1)
            def _(n=n):
                add_to(theirs, held, n)


def final_kernel(me_ref, column, row, row_there, from_1, from_3, from_2, head, out_ref):
    sums = column[...] + jnp.where((me_ref[0] & 1) == 0, row[...], row_there[...])
    numerator, denominator = sums[:, 0:D], sums[:, D : D + 1]
    for piece in (from_1, from_3, from_2):
        numerator += piece[:, 0:D].astype(F32)
        denominator += total_of(piece[:, D:MSG].astype(F32))
    joined = (numerator / denominator).astype(BF16)
    out_ref[0] = matmul(joined, head[...]).astype(BF16)


def params(mib):
    return pltpu.CompilerParams(vmem_limit_bytes=mib * 2**20)


def shards(
    encoder_tokens,
    pair_list,
    pair_count,
    embed_weight,
    self_gain,
    self_qkv,
    self_out,
    cross_gain,
    cross_qkv,
    cross_out,
    mlp_gain,
    mlp_up,
    mlp_down,
    conf_weight,
    head_weight,
):
    me = lax.axis_index("row") * 8 + lax.axis_index("col")
    core = me & 1

    up_out, down_out = (lax.dynamic_index_in_dim(w, 1 - core, 0, False) for w in (mlp_up, mlp_down))
    came = swap(jnp.stack([up_out, down_out]))
    up_own, down_own = (lax.dynamic_index_in_dim(w, core, 0, False) for w in (mlp_up, mlp_down))
    mine = jnp.concatenate([pair_list.reshape(4), pair_count.reshape(1)])
    theirs = swap(mine)
    far = send(mine, ((Z, 1),), ((X, 1),))
    ids = (me.reshape(1), mine, theirs)

    own = jnp.einsum(
        "td,de->te", encoder_tokens[0], embed_weight, preferred_element_type=F32
    ).astype(BF16)

    block = jnp.concatenate([jnp.stack([up_own, down_own]), came], axis=1)
    block = join(block.reshape(96, D), own)[None]
    line = join(block, send(block, ((Y, 1),), ((Y, 3),)))
    line_far = send(line, ((Y, 3),), ((Y, 1),))

    def over_plane(held, first, last, one, two):
        near = send(held, ((first, 1),), ((first, 3),))
        held = join(held[:, :96], near[:, :96])
        held = join(held, send(held, ((first, 3),), ((first, 1),)))
        near = send(held, ((last, one),), ((last, two),))
        half = lax.dynamic_slice_in_dim(held, ((me >> 1) & 1) * 4, 4, 0)
        far = send(half, ((last, two),), ((last, one),))
        rest = send(far, ((Y, 1),), ((Y, 3),))
        across = send(near, ((last, two),), ((last, one),))
        return [h.reshape(-1, 2, 48, D) for h in (held, near, far, rest, across)]

    weights_a = over_plane(line, X, Z, 3, 1)
    weights_b = over_plane(line_far, Z, X, 1, 3)

    tokens = own[None]
    tokens = join(tokens, send(tokens, ((X, 1),), ((Z, 1),)))
    tokens = join(tokens, send(tokens, ((X, 3),), ((Z, 3),)))
    tokens = join(tokens, send(tokens, ((Z, 3),), ((X, 3),)))
    picked = pl.pallas_call(
        pick_kernel,
        out_shape=jax.ShapeDtypeStruct((2, T, D), BF16),
        in_specs=[SMEM] * 2 + [HBM],
        out_specs=VMEM,
        scratch_shapes=[pltpu.SemaphoreType.DMA((2,))],
        name="pick",
    )(ids[0], far, *in_hbm(tokens))
    tokens_far = send(picked, ((Z, 1),), ((X, 1),))
    selected = pl.pallas_call(
        select_kernel,
        out_shape=jax.ShapeDtypeStruct((5, T, D), BF16),
        in_specs=[SMEM] * 3 + [HBM] * 4 + [VMEM],
        out_specs=VMEM,
        scratch_shapes=[pltpu.SemaphoreType.DMA((4,))],
        name="select",
    )(*ids, *in_hbm(tokens, tokens_far, line, line_far), own)
    received = swap(selected)

    after, mlp_in = pl.pallas_call(
        attend_kernel,
        out_shape=[jax.ShapeDtypeStruct((SLOTS * T, D), BF16)] * 2,
        in_specs=[SMEM] * 3 + [VMEM] * 5 + [HBM] * 4,
        out_specs=[VMEM, VMEM],
        scratch_shapes=ATT_SCRATCH,
        compiler_params=params(32),
        name="attend",
    )(
        *ids,
        selected,
        received,
        self_gain,
        cross_gain.reshape(4, D),
        mlp_gain,
        *in_hbm(self_qkv, self_out, cross_qkv, cross_out),
    )

    def held_weights(groups):
        return [pltpu.VMEM((len(groups), 8, 2, 48, D), BF16), pltpu.SemaphoreType.DMA((sum(groups),))]

    early, late = (1, 1, 1, 1, 2), (2, 1, 1)

    sums = jax.ShapeDtypeStruct((SLOTS * T, D), F32)
    partial = pl.pallas_call(
        functools.partial(mlp_kernel, early),
        out_shape=sums,
        in_specs=[VMEM] * 2 + [HBM] * sum(early),
        out_specs=VMEM,
        scratch_shapes=held_weights(early),
        compiler_params=params(32),
        name="lift",
    )(
        after,
        mlp_in,
        *(weights_a[0], weights_b[0], weights_a[1], weights_b[1], weights_a[2], weights_a[3]),
    )
    msg = lambda *shape: jax.ShapeDtypeStruct((*shape, MSG), BF16)
    piece_own, piece_a, piece_b = pl.pallas_call(
        functools.partial(mlp_last_kernel, late),
        out_shape=[msg(2, T)] * 3,
        in_specs=[SMEM] * 3 + [VMEM] * 3 + [HBM] * sum(late),
        out_specs=[VMEM] * 3,
        scratch_shapes=[pltpu.VMEM((SLOTS * T, D), F32), pltpu.VMEM((SLOTS, T, MSG), BF16)]
        + held_weights(late),
        compiler_params=params(32),
        name="last",
    )(
        *ids,
        partial,
        mlp_in,
        conf_weight.reshape(1, D),
        *(weights_b[2], weights_b[3], weights_a[4], weights_b[4]),
    )

    masks = (1, 3, 2)
    got_a = [swap(piece_a)]
    got_a += [send(piece_a, ((C, 1),), ((X, m), (C, 1))) for m in masks]
    got_b = [send(piece_b, ((Y, m),), ((Z, m),)) for m in masks]
    pieces = in_hbm(*got_a, piece_b, *got_b)
    summed = jax.ShapeDtypeStruct((T, MSG), F32)
    column, *parts = pl.pallas_call(
        middle_kernel,
        out_shape=[summed] + [msg(T)] * 3,
        in_specs=[SMEM] + [HBM] * 8,
        out_specs=[VMEM] * 4,
        scratch_shapes=[
            pltpu.VMEM((5, T, MSG), F32),
            pltpu.VMEM((8, T, MSG), BF16),
            pltpu.SemaphoreType.DMA((4,)),
        ],
        name="middle",
    )(ids[0], *pieces)
    last = [send(s, ((Z, m),), ((X, m),)) for s, m in zip(parts, masks)]
    row, row_out = pl.pallas_call(
        row_kernel,
        out_shape=[summed] * 2,
        in_specs=[SMEM] + [HBM] * 5,
        out_specs=[VMEM] * 2,
        scratch_shapes=[pltpu.VMEM((10, T, MSG), BF16), pltpu.SemaphoreType.DMA((5,))],
        name="rows",
    )(ids[0], *in_hbm(piece_own), *pieces[4:])
    row_there = swap(row_out)
    return pl.pallas_call(
        final_kernel,
        out_shape=jax.ShapeDtypeStruct((1, T, 1024), BF16),
        in_specs=[SMEM] + [VMEM] * 7,
        out_specs=VMEM,
        name="head",
    )(ids[0], column, row, row_there, *last, head_weight)


def solution(mesh):
    return jax.shard_map(
        shards,
        mesh=mesh,
        in_specs=(
            P(("row", "col"), None, None),
            P("row", "col", None, None),
            P("row", "col"),
            P(),
            P(),
            P(),
            P(),
            P(),
            P(),
            P(),
            P(),
            P(None, ("row", "col"), None),
            P(None, ("row", "col"), None),
            P(),
            P(),
        ),
        out_specs=P(("row", "col"), None, None),
        check_vma=False,
    )
```

```python
import functools

import jax
import jax.numpy as jnp
from jax import lax
from jax.experimental import pallas as pl
from jax.experimental.pallas import tpu as pltpu
from jax.sharding import PartitionSpec as P


HEADS = 12
HEAD_DIM = 64
NORM_EPSILON = 1e-05
D = 768
T = 64
SLOTS = 4
AUX = 128
MSG = D + AUX
F32 = jnp.float32
BF16 = jnp.bfloat16
AXES = ("row", "col")


def coords(i):
    return i // 32, (i // 8) % 4, (i // 2) % 4, i % 2


def linear(z, x, y, c):
    return ((z * 4 + x) * 4 + y) * 2 + c


Z, X, Y, C = 0, 1, 2, 3


def send(array, core0, core1):
    pairs = []
    for i in range(128):
        at = list(coords(i))
        for dim, mask in (core0, core1)[at[3]]:
            at[dim] ^= mask
        pairs.append((i, linear(*at)))
    return lax.ppermute(array, AXES, pairs)


def swap(array):
    return send(array, ((C, 1),), ((C, 1),))


def join(*arrays):
    return jnp.concatenate(arrays, axis=0)


def place(delta, order):
    found = jnp.int32(0)
    for at, mask in enumerate(order):
        found = jnp.where(delta == mask, at, found)
    return found


def coordinates(me):
    return me >> 5, (me >> 3) & 3, (me >> 1) & 3, me & 1


VMEM = pl.BlockSpec(memory_space=pltpu.VMEM)
SMEM = pl.BlockSpec(memory_space=pltpu.SMEM)
HBM = pl.BlockSpec(memory_space=pltpu.HBM)


def in_hbm(*arrays):
    return [pltpu.with_memory_space_constraint(a, pltpu.HBM) for a in arrays]


def seconds_at(ids_ref, z, x, core):
    found = []
    for second in (ids_ref[1], ids_ref[3]):
        to_z, to_x, _, _ = coordinates(second)
        last = jnp.where(core == 0, z ^ to_z, x ^ to_x)
        first = jnp.where(core == 0, x ^ to_x, z ^ to_z)
        found.append((last, (last >> 1) * 4 + place(first, (0, 1, 3, 2))))
    return found


def pick_kernel(me_ref, far_ref, tokens, out_ref, sems):
    z, x, _, core = coordinates(me_ref[0])
    copies = [
        pltpu.make_async_copy(tokens.at[at], out_ref.at[n], sems.at[n])
        for n, (_, at) in enumerate(seconds_at(far_ref, z, x, core))
    ]
    for copy in copies:
        copy.start()
    for copy in copies:
        copy.wait()


def select_kernel(me_ref, ids_ref, tokens, tokens_far, line, line_far, own, out_ref, sems):
    z, x, y, core = coordinates(me_ref[0])
    for n, (last, at) in enumerate(seconds_at(ids_ref, z, x, core)):

        @pl.when((last == 0) | (last == 3))
        def _(n=n, at=at):
            pltpu.make_async_copy(tokens.at[at], out_ref.at[n], sems.at[n]).start()

        @pl.when((last == 1) | (last == 2))
        def _(n=n):
            pltpu.make_async_copy(tokens_far.at[n], out_ref.at[n], sems.at[n]).start()

    for n, first in ((2, ids_ref[2]), (3, ids_ref[7])):
        delta = y ^ ((first >> 1) & 3)
        at = jnp.where(core == 0, place(delta, (0, 1, 3, 2)), place(delta, (0, 3, 1, 2)))

        @pl.when(at < 2)
        def _(n=n, at=at):
            pltpu.make_async_copy(line.at[at, pl.ds(96, T)], out_ref.at[n], sems.at[n]).start()

        @pl.when(at >= 2)
        def _(n=n, at=at):
            pltpu.make_async_copy(line_far.at[at - 2, pl.ds(96, T)], out_ref.at[n], sems.at[n]).start()

    out_ref[4] = own[...]
    for n in range(4):
        pltpu.make_async_copy(own, out_ref.at[n], sems.at[n]).wait()


def normed(values, gain):
    values = values.astype(F32)
    centered = values - jnp.mean(values, -1, keepdims=True)
    variance = jnp.mean(centered * centered, -1, keepdims=True)
    return (centered * lax.rsqrt(variance + NORM_EPSILON) * gain).astype(BF16)


def matmul(a, b):
    return lax.dot_general(a, b, (((1,), (0,)), ((), ())), preferred_element_type=F32)


def attention(qkv_ref, score_ref, expo_ref, out_ref):
    pairs = HEADS // 2
    left = lax.broadcasted_iota(jnp.int32, (T, 128), 1) < HEAD_DIM
    same = (lax.broadcasted_iota(jnp.int32, (128, 128), 0) < HEAD_DIM) == (
        lax.broadcasted_iota(jnp.int32, (128, 128), 1) < HEAD_DIM
    )
    ones = jnp.where(same, 1.0, 0.0).astype(BF16)

    def rows_of(slot):
        return pl.ds(slot * T, T)

    def split(both):
        zero = jnp.zeros_like(both)
        return jnp.concatenate([jnp.where(left, both, zero), jnp.where(left, zero, both)], axis=0)

    def score(slot, carry):
        for pair in range(pairs):
            q = qkv_ref[rows_of(slot), pl.ds(pair * 128, 128)]
            k = split(qkv_ref[rows_of(slot), pl.ds(D + pair * 128, 128)])
            score_ref[slot * pairs + pair] = lax.dot_general(
                q, k, (((1,), (1,)), ((), ())), preferred_element_type=F32
            )
        return carry

    def exponent(slot, carry):
        for pair in range(pairs):
            scores = score_ref[slot * pairs + pair] * 0.125
            high_left = jnp.max(jnp.where(left, scores, -jnp.inf), 1, keepdims=True)
            high_right = jnp.max(jnp.where(left, -jnp.inf, scores), 1, keepdims=True)
            expo = jnp.exp(scores - jnp.where(left, high_left, high_right))
            expo_ref[slot * pairs + pair] = expo.astype(BF16)
        return carry

    def weigh(slot, carry):
        for pair in range(pairs):
            expo = expo_ref[slot * pairs + pair]
            v = split(qkv_ref[rows_of(slot), pl.ds(2 * D + pair * 128, 128)])
            out_ref[rows_of(slot), pl.ds(pair * 128, 128)] = (
                matmul(expo, v) * (1.0 / matmul(expo, ones))
            ).astype(BF16)
        return carry

    for stage in (score, exponent, weigh):
        for slot in range(SLOTS):
            stage(slot, 0)


ATT_SCRATCH = [
    pltpu.VMEM((SLOTS * T, D), BF16),
    pltpu.VMEM((SLOTS * T, D), BF16),
    pltpu.VMEM((SLOTS * T, 3 * D), BF16),
    pltpu.VMEM((SLOTS * T, D), BF16),
    pltpu.VMEM((SLOTS * HEADS // 2, T, 128), F32),
    pltpu.VMEM((SLOTS * HEADS // 2, T, 128), BF16),
    pltpu.VMEM((D, 3 * D), BF16),
    pltpu.VMEM((D, D), BF16),
    pltpu.VMEM((D, 3 * D), BF16),
    pltpu.VMEM((D, D), BF16),
    pltpu.SemaphoreType.DMA((4,)),
]


def attend_kernel(
    me_ref,
    ids_ref,
    local_ref,
    recv_ref,
    self_gain_ref,
    cross_gain_ref,
    mlp_gain_ref,
    self_qkv_hbm,
    self_out_hbm,
    cross_qkv_hbm,
    cross_out_hbm,
    after_ref,
    mlp_in_ref,
    x_ref,
    y_ref,
    qkv_ref,
    att_ref,
    score_ref,
    expo_ref,
    self_qkv,
    self_out,
    cross_qkv,
    cross_out,
    sems,
):
    side = me_ref[0] & 1
    copies = [
        pltpu.make_async_copy(src.at[side], dst, sems.at[n])
        for n, (src, dst) in enumerate(
            (
                (self_qkv_hbm, self_qkv),
                (self_out_hbm, self_out),
                (cross_qkv_hbm, cross_qkv),
                (cross_out_hbm, cross_out),
            )
        )
    ]
    for copy in copies:
        copy.start()

    def place(first_ref, second_ref):
        first_ref[0:64] = local_ref[4]
        first_ref[64:128] = jnp.where((ids_ref[2] & 1) == side, local_ref[2], recv_ref[3])
        first_ref[128:192] = recv_ref[4]
        first_ref[192:256] = jnp.where((ids_ref[7] & 1) == side, local_ref[3], recv_ref[2])
        second_ref[0:64] = local_ref[0]
        second_ref[64:128] = local_ref[1]
        second_ref[128:192] = recv_ref[0]
        second_ref[192:256] = recv_ref[1]

    @pl.when(side == 0)
    def _():
        place(x_ref, y_ref)

    @pl.when(side == 1)
    def _():
        place(y_ref, x_ref)

    xn = normed(x_ref[...], self_gain_ref[pl.ds(side, 1), :])
    copies[0].wait()
    qkv_ref[...] = matmul(xn, self_qkv[...]).astype(BF16)
    attention(qkv_ref, score_ref, expo_ref, att_ref)
    copies[1].wait()
    after_self = (x_ref[...].astype(F32) + matmul(att_ref[...], self_out[...])).astype(BF16)
    x_ref[...] = after_self
    qn = normed(after_self, cross_gain_ref[pl.ds(2 * side, 1), :])
    yn = normed(y_ref[...], cross_gain_ref[pl.ds(2 * side + 1, 1), :])
    copies[2].wait()
    qkv_ref[:, 0:D] = matmul(qn, cross_qkv[:, 0:D]).astype(BF16)
    qkv_ref[:, D : 3 * D] = matmul(yn, cross_qkv[:, D : 3 * D]).astype(BF16)
    attention(qkv_ref, score_ref, expo_ref, att_ref)
    copies[3].wait()
    after_cross = (x_ref[...].astype(F32) + matmul(att_ref[...], cross_out[...])).astype(BF16)
    after_ref[...] = after_cross
    mlp_in_ref[...] = normed(after_cross, mlp_gain_ref[pl.ds(side, 1), :])


def gelu(v):
    return v * (lax.erf(v * 0.7071067811865476) + 1.0) * 0.5


def accumulate(groups, mlp_in_ref, weights, acc_ref, held, sems):
    copies, at = [], 0
    for n, size in enumerate(groups):
        blocks = []
        for m in range(size):
            part = slice(m * 8 // size, (m + 1) * 8 // size)
            to = held.at[n, pl.ds(part.start, part.stop - part.start)]
            blocks.append(pltpu.make_async_copy(weights[at], to, sems.at[at]))
            at += 1
        copies.append(blocks)
    for blocks in copies:
        for copy in blocks:
            copy.start()
    for n, blocks in enumerate(copies):
        for copy in blocks:
            copy.wait()
        up = held[n, :, 0].reshape(384, D)
        down = held[n, :, 1].reshape(384, D)
        lifted = lax.dot_general(
            mlp_in_ref[...], up, (((1,), (1,)), ((), ())), preferred_element_type=F32
        )
        acc_ref[...] += matmul(gelu(lifted).astype(BF16), down)


def mlp_kernel(groups, after_ref, mlp_in_ref, *refs):
    count = sum(groups)
    acc_ref, held, sems = refs[count:]
    acc_ref[...] = after_ref[...].astype(F32)
    accumulate(groups, mlp_in_ref, refs[:count], acc_ref, held, sems)


def mlp_last_kernel(groups, me_ref, ids_ref, before_ref, mlp_in_ref, conf_ref, *refs):
    count = sum(groups)
    own_ref, a_ref, b_ref, acc_ref, message, held, sems = refs[count:]
    acc_ref[...] = before_ref[...]
    accumulate(groups, mlp_in_ref, refs[:count], acc_ref, held, sems)
    decoded = acc_ref[...].astype(BF16)
    conf = 1.0 + jnp.exp(jnp.sum(decoded.astype(F32) * conf_ref[...], -1, keepdims=True))
    high = conf.astype(BF16)
    rest = conf - high.astype(F32)
    middle = rest.astype(BF16)
    low = (rest - middle.astype(F32)).astype(BF16)
    lane = lax.broadcasted_iota(jnp.int32, (T, AUX), 1)
    side = me_ref[0] & 1
    for slot in range(SLOTS):
        rows = slice(slot * T, slot * T + T)
        at = 5 * (slot // 2)
        first, second = ids_ref[at + 2 * (slot % 2)], ids_ref[at + 2 * (slot % 2) + 1]
        owner = jnp.where(slot % 2 < ids_ref[at + 4], jnp.where(side == 0, first, second), -1).astype(F32)
        aux = jnp.where(lane == 0, owner, 0.0)
        aux = jnp.where(lane == 1, high[rows].astype(F32), aux)
        aux = jnp.where(lane == 2, middle[rows].astype(F32), aux)
        aux = jnp.where(lane == 3, low[rows].astype(F32), aux)
        message[slot, :, 0:D] = decoded[rows]
        message[slot, :, D:MSG] = aux.astype(BF16)

    def put(ref, slots):
        for n, slot in enumerate(slots):
            ref[n] = message[slot]

    @pl.when(side == 0)
    def _():
        put(own_ref, (0, 2))
        put(a_ref, (1, 3))
        put(b_ref, (1, 3))

    @pl.when(side == 1)
    def _():
        put(own_ref, (0, 2))
        put(a_ref, (2, 3))
        put(b_ref, (0, 1))


def total_of(aux):
    return aux[:, 1:2] + aux[:, 2:3] + aux[:, 3:4]


def owner_of(ref, slot):
    lane = lax.broadcasted_iota(jnp.int32, (16, AUX), 1)
    aux = ref[slot, 0:16, D:MSG].astype(F32)
    return jnp.max(jnp.where(lane == 0, aux, -1.0)).astype(jnp.int32)


def add_to(sums, ref, slot):
    conf = total_of(ref[slot, :, D:MSG].astype(F32))
    sums[:, 0:D] += conf * ref[slot, :, 0:D].astype(F32)
    sums[:, D:MSG] += jnp.broadcast_to(conf, (T, AUX))


def load(sources, held, sems):
    copies = [
        pltpu.make_async_copy(src, held.at[pl.ds(2 * n, 2)], sems.at[n]) for n, src in enumerate(sources)
    ]
    for copy in copies:
        copy.start()
    return copies


def middle_kernel(me_ref, *refs):
    out_0 = refs[8]
    outs = refs[9:12]
    sums, held, sems = refs[12:]
    z, x, _, core = coordinates(me_ref[0])

    @pl.when(core == 0)
    def _():
        load(refs[0:4], held, sems)

    @pl.when(core == 1)
    def _():
        load(refs[4:8], held, sems)

    copies = [pltpu.make_async_copy(refs[n], held.at[pl.ds(2 * n, 2)], sems.at[n]) for n in range(4)]
    sums[0:4] = jnp.zeros((4, T, MSG), F32)
    for n in range(8):
        if n % 2 == 0:
            copies[n // 2].wait()
        owner = owner_of(held, n)
        to_z, to_x, _, _ = coordinates(owner)
        here = jnp.where(core == 0, to_x == x, to_z == z)
        to = jnp.where(core == 0, to_z ^ z, to_x ^ x)
        add_to(sums.at[jnp.where((owner >= 0) & here, to, 4)], held, n)

    out_0[...] = sums[0]
    lane = lax.broadcasted_iota(jnp.int32, (T, AUX), 1)
    for mask, out in zip((1, 3, 2), outs):
        out[:, 0:D] = sums[mask, :, 0:D].astype(BF16)
        denominator = sums[mask, :, D:MSG]
        high = denominator.astype(BF16)
        rest = denominator - high.astype(F32)
        middle = rest.astype(BF16)
        low = rest - middle.astype(F32)
        aux = jnp.where(lane == 1, high.astype(F32), 0.0)
        aux = jnp.where(lane == 2, middle.astype(F32), aux)
        out[:, D:MSG] = jnp.where(lane == 3, low, aux).astype(BF16)


def row_kernel(me_ref, *refs):
    mine, theirs, held, sems = refs[5:]
    me = me_ref[0]
    mine[...] = jnp.zeros((T, MSG), F32)
    theirs[...] = jnp.zeros((T, MSG), F32)

    @pl.when((me & 1) == 0)
    def _():
        copies = load(refs[:5], held, sems)
        for n in range(10):
            if n % 2 == 0:
                copies[n // 2].wait()
            owner = owner_of(held, n)

            @pl.when(owner == me)
            def _(n=n):
                add_to(mine, held, n)

            @pl.when(owner == me + 1)
            def _(n=n):
                add_to(theirs, held, n)


def final_kernel(me_ref, column, row, row_there, from_1, from_3, from_2, head, out_ref):
    sums = column[...] + jnp.where((me_ref[0] & 1) == 0, row[...], row_there[...])
    numerator, denominator = sums[:, 0:D], sums[:, D : D + 1]
    for piece in (from_1, from_3, from_2):
        numerator += piece[:, 0:D].astype(F32)
        denominator += total_of(piece[:, D:MSG].astype(F32))
    joined = (numerator / denominator).astype(BF16)
    out_ref[0] = matmul(joined, head[...]).astype(BF16)


def params(mib):
    return pltpu.CompilerParams(vmem_limit_bytes=mib * 2**20)


def shards(
    encoder_tokens,
    pair_list,
    pair_count,
    embed_weight,
    self_gain,
    self_qkv,
    self_out,
    cross_gain,
    cross_qkv,
    cross_out,
    mlp_gain,
    mlp_up,
    mlp_down,
    conf_weight,
    head_weight,
):
    me = lax.axis_index("row") * 8 + lax.axis_index("col")
    core = me & 1

    up_out, down_out = (lax.dynamic_index_in_dim(w, 1 - core, 0, False) for w in (mlp_up, mlp_down))
    came = swap(jnp.stack([up_out, down_out]))
    up_own, down_own = (lax.dynamic_index_in_dim(w, core, 0, False) for w in (mlp_up, mlp_down))
    mine = jnp.concatenate([pair_list.reshape(4), pair_count.reshape(1)])
    theirs = swap(mine)
    far = send(mine, ((Z, 1),), ((X, 1),))
    ids = (me.reshape(1), jnp.concatenate([mine, theirs]))

    own = jnp.einsum(
        "td,de->te", encoder_tokens[0], embed_weight, preferred_element_type=F32
    ).astype(BF16)

    block = jnp.concatenate([jnp.stack([up_own, down_own]), came], axis=1)
    block = join(block.reshape(96, D), own)[None]
    line = join(block, send(block, ((Y, 1),), ((Y, 3),)))
    line_far = send(line, ((Y, 3),), ((Y, 1),))

    def over_plane(held, first, last, one, two):
        near = send(held, ((first, 1),), ((first, 3),))
        held = join(held[:, :96], near[:, :96])
        held = join(held, send(held, ((first, 3),), ((first, 1),)))
        near = send(held, ((last, one),), ((last, two),))
        half = lax.dynamic_slice_in_dim(held, ((me >> 1) & 1) * 4, 4, 0)
        far = send(half, ((last, two),), ((last, one),))
        rest = send(far, ((Y, 1),), ((Y, 3),))
        across = send(near, ((last, two),), ((last, one),))
        return [h.reshape(-1, 2, 48, D) for h in (held, near, far, rest, across)]

    weights_a = over_plane(line, X, Z, 3, 1)
    weights_b = over_plane(line_far, Z, X, 1, 3)

    tokens = own[None]
    tokens = join(tokens, send(tokens, ((X, 1),), ((Z, 1),)))
    tokens = join(tokens, send(tokens, ((X, 3),), ((Z, 3),)))
    tokens = join(tokens, send(tokens, ((Z, 3),), ((X, 3),)))
    picked = pl.pallas_call(
        pick_kernel,
        out_shape=jax.ShapeDtypeStruct((2, T, D), BF16),
        in_specs=[SMEM] * 2 + [HBM],
        out_specs=VMEM,
        scratch_shapes=[pltpu.SemaphoreType.DMA((2,))],
        name="pick",
    )(ids[0], far, *in_hbm(tokens))
    tokens_far = send(picked, ((Z, 1),), ((X, 1),))
    selected = pl.pallas_call(
        select_kernel,
        out_shape=jax.ShapeDtypeStruct((5, T, D), BF16),
        in_specs=[SMEM] * 2 + [HBM] * 4 + [VMEM],
        out_specs=VMEM,
        scratch_shapes=[pltpu.SemaphoreType.DMA((4,))],
        name="select",
    )(*ids, *in_hbm(tokens, tokens_far, line, line_far), own)
    received = swap(selected)

    after, mlp_in = pl.pallas_call(
        attend_kernel,
        out_shape=[jax.ShapeDtypeStruct((SLOTS * T, D), BF16)] * 2,
        in_specs=[SMEM] * 2 + [VMEM] * 5 + [HBM] * 4,
        out_specs=[VMEM, VMEM],
        scratch_shapes=ATT_SCRATCH,
        compiler_params=params(32),
        name="attend",
    )(
        *ids,
        selected,
        received,
        self_gain,
        cross_gain.reshape(4, D),
        mlp_gain,
        *in_hbm(self_qkv, self_out, cross_qkv, cross_out),
    )

    def held_weights(groups):
        return [pltpu.VMEM((len(groups), 8, 2, 48, D), BF16), pltpu.SemaphoreType.DMA((sum(groups),))]

    early, late = (1, 1, 1, 1, 2), (2, 1, 1)

    sums = jax.ShapeDtypeStruct((SLOTS * T, D), F32)
    partial = pl.pallas_call(
        functools.partial(mlp_kernel, early),
        out_shape=sums,
        in_specs=[VMEM] * 2 + [HBM] * sum(early),
        out_specs=VMEM,
        scratch_shapes=held_weights(early),
        compiler_params=params(32),
        name="lift",
    )(
        after,
        mlp_in,
        *(weights_a[0], weights_b[0], weights_a[1], weights_b[1], weights_a[2], weights_a[3]),
    )
    msg = lambda *shape: jax.ShapeDtypeStruct((*shape, MSG), BF16)
    piece_own, piece_a, piece_b = pl.pallas_call(
        functools.partial(mlp_last_kernel, late),
        out_shape=[msg(2, T)] * 3,
        in_specs=[SMEM] * 2 + [VMEM] * 3 + [HBM] * sum(late),
        out_specs=[VMEM] * 3,
        scratch_shapes=[pltpu.VMEM((SLOTS * T, D), F32), pltpu.VMEM((SLOTS, T, MSG), BF16)]
        + held_weights(late),
        compiler_params=params(32),
        name="last",
    )(
        *ids,
        partial,
        mlp_in,
        conf_weight.reshape(1, D),
        *(weights_b[2], weights_b[3], weights_a[4], weights_b[4]),
    )

    masks = (1, 3, 2)
    got_a = [swap(piece_a)]
    got_a += [send(piece_a, ((C, 1),), ((X, m), (C, 1))) for m in masks]
    got_b = [send(piece_b, ((Y, m),), ((Z, m),)) for m in masks]
    pieces = in_hbm(*got_a, piece_b, *got_b)
    summed = jax.ShapeDtypeStruct((T, MSG), F32)
    column, *parts = pl.pallas_call(
        middle_kernel,
        out_shape=[summed] + [msg(T)] * 3,
        in_specs=[SMEM] + [HBM] * 8,
        out_specs=[VMEM] * 4,
        scratch_shapes=[
            pltpu.VMEM((5, T, MSG), F32),
            pltpu.VMEM((8, T, MSG), BF16),
            pltpu.SemaphoreType.DMA((4,)),
        ],
        name="middle",
    )(ids[0], *pieces)
    last = [send(s, ((Z, m),), ((X, m),)) for s, m in zip(parts, masks)]
    row, row_out = pl.pallas_call(
        row_kernel,
        out_shape=[summed] * 2,
        in_specs=[SMEM] + [HBM] * 5,
        out_specs=[VMEM] * 2,
        scratch_shapes=[pltpu.VMEM((10, T, MSG), BF16), pltpu.SemaphoreType.DMA((5,))],
        name="rows",
    )(ids[0], *in_hbm(piece_own), *pieces[4:])
    row_there = swap(row_out)
    return pl.pallas_call(
        final_kernel,
        out_shape=jax.ShapeDtypeStruct((1, T, 1024), BF16),
        in_specs=[SMEM] + [VMEM] * 7,
        out_specs=VMEM,
        name="head",
    )(ids[0], column, row, row_there, *last, head_weight)


def solution(mesh):
    return jax.shard_map(
        shards,
        mesh=mesh,
        in_specs=(
            P(("row", "col"), None, None),
            P("row", "col", None, None),
            P("row", "col"),
            P(),
            P(),
            P(),
            P(),
            P(),
            P(),
            P(),
            P(),
            P(None, ("row", "col"), None),
            P(None, ("row", "col"), None),
            P(),
            P(),
        ),
        out_specs=P(("row", "col"), None, None),
        check_vma=False,
    )
```

```python
import functools

import jax
import jax.numpy as jnp
from jax import lax
from jax.experimental import pallas as pl
from jax.experimental.pallas import tpu as pltpu
from jax.sharding import PartitionSpec as P


HEADS = 12
HEAD_DIM = 64
NORM_EPSILON = 1e-05
D = 768
T = 64
SLOTS = 4
AUX = 128
MSG = D + AUX
F32 = jnp.float32
BF16 = jnp.bfloat16
AXES = ("row", "col")


def coords(i):
    return i // 32, (i // 8) % 4, (i // 2) % 4, i % 2


def linear(z, x, y, c):
    return ((z * 4 + x) * 4 + y) * 2 + c


Z, X, Y, C = 0, 1, 2, 3


def send(array, core0, core1):
    pairs = []
    for i in range(128):
        at = list(coords(i))
        for dim, mask in (core0, core1)[at[3]]:
            at[dim] ^= mask
        pairs.append((i, linear(*at)))
    return lax.ppermute(array, AXES, pairs)


def swap(array):
    return send(array, ((C, 1),), ((C, 1),))


def join(*arrays):
    return jnp.concatenate(arrays, axis=0)


def place(delta, order):
    found = jnp.int32(0)
    for at, mask in enumerate(order):
        found = jnp.where(delta == mask, at, found)
    return found


def coordinates(me):
    return me >> 5, (me >> 3) & 3, (me >> 1) & 3, me & 1


VMEM = pl.BlockSpec(memory_space=pltpu.VMEM)
SMEM = pl.BlockSpec(memory_space=pltpu.SMEM)
HBM = pl.BlockSpec(memory_space=pltpu.HBM)


def in_hbm(*arrays):
    return [pltpu.with_memory_space_constraint(a, pltpu.HBM) for a in arrays]


def seconds_at(ids_ref, z, x, core):
    found = []
    for second in (ids_ref[1], ids_ref[3]):
        to_z, to_x, _, _ = coordinates(second)
        last = jnp.where(core == 0, z ^ to_z, x ^ to_x)
        first = jnp.where(core == 0, x ^ to_x, z ^ to_z)
        found.append((last, (last >> 1) * 4 + place(first, (0, 1, 3, 2))))
    return found


def pick_kernel(me_ref, far_ref, tokens, out_ref, sems):
    z, x, _, core = coordinates(me_ref[0])
    copies = [
        pltpu.make_async_copy(tokens.at[at], out_ref.at[n], sems.at[n])
        for n, (_, at) in enumerate(seconds_at(far_ref, z, x, core))
    ]
    for copy in copies:
        copy.start()
    for copy in copies:
        copy.wait()


def select_kernel(me_ref, ids_ref, tokens, tokens_far, line, line_far, own, out_ref, sems):
    z, x, y, core = coordinates(me_ref[0])
    for n, (last, at) in enumerate(seconds_at(ids_ref, z, x, core)):

        @pl.when((last == 0) | (last == 3))
        def _(n=n, at=at):
            pltpu.make_async_copy(tokens.at[at], out_ref.at[n], sems.at[n]).start()

        @pl.when((last == 1) | (last == 2))
        def _(n=n):
            pltpu.make_async_copy(tokens_far.at[n], out_ref.at[n], sems.at[n]).start()

    for n, first in ((2, ids_ref[2]), (3, ids_ref[7])):
        delta = y ^ ((first >> 1) & 3)
        at = jnp.where(core == 0, place(delta, (0, 1, 3, 2)), place(delta, (0, 3, 1, 2)))

        @pl.when(at < 2)
        def _(n=n, at=at):
            pltpu.make_async_copy(line.at[at, pl.ds(96, T)], out_ref.at[n], sems.at[n]).start()

        @pl.when(at >= 2)
        def _(n=n, at=at):
            pltpu.make_async_copy(line_far.at[at - 2, pl.ds(96, T)], out_ref.at[n], sems.at[n]).start()

    out_ref[4] = own[...]
    for n in range(4):
        pltpu.make_async_copy(own, out_ref.at[n], sems.at[n]).wait()


def normed(values, gain):
    values = values.astype(F32)
    centered = values - jnp.mean(values, -1, keepdims=True)
    variance = jnp.mean(centered * centered, -1, keepdims=True)
    return (centered * lax.rsqrt(variance + NORM_EPSILON) * gain).astype(BF16)


def matmul(a, b):
    return lax.dot_general(a, b, (((1,), (0,)), ((), ())), preferred_element_type=F32)


def attention(qkv_ref, score_ref, expo_ref, out_ref):
    pairs = HEADS // 2
    left = lax.broadcasted_iota(jnp.int32, (T, 128), 1) < HEAD_DIM
    same = (lax.broadcasted_iota(jnp.int32, (128, 128), 0) < HEAD_DIM) == (
        lax.broadcasted_iota(jnp.int32, (128, 128), 1) < HEAD_DIM
    )
    ones = jnp.where(same, 1.0, 0.0).astype(BF16)

    def rows_of(slot):
        return pl.ds(slot * T, T)

    def split(both):
        zero = jnp.zeros_like(both)
        return jnp.concatenate([jnp.where(left, both, zero), jnp.where(left, zero, both)], axis=0)

    def score(slot, carry):
        for pair in range(pairs):
            q = qkv_ref[rows_of(slot), pl.ds(pair * 128, 128)]
            k = split(qkv_ref[rows_of(slot), pl.ds(D + pair * 128, 128)])
            score_ref[slot * pairs + pair] = lax.dot_general(
                q, k, (((1,), (1,)), ((), ())), preferred_element_type=F32
            )
        return carry

    def exponent(slot, carry):
        for pair in range(pairs):
            scores = score_ref[slot * pairs + pair] * 0.125
            high_left = jnp.max(jnp.where(left, scores, -jnp.inf), 1, keepdims=True)
            high_right = jnp.max(jnp.where(left, -jnp.inf, scores), 1, keepdims=True)
            expo = jnp.exp(scores - jnp.where(left, high_left, high_right))
            expo_ref[slot * pairs + pair] = expo.astype(BF16)
        return carry

    def weigh(slot, carry):
        for pair in range(pairs):
            expo = expo_ref[slot * pairs + pair]
            v = split(qkv_ref[rows_of(slot), pl.ds(2 * D + pair * 128, 128)])
            out_ref[rows_of(slot), pl.ds(pair * 128, 128)] = (
                matmul(expo, v) * (1.0 / matmul(expo, ones))
            ).astype(BF16)
        return carry

    for stage in (score, exponent, weigh):
        for slot in range(SLOTS):
            stage(slot, 0)


ATT_SCRATCH = [
    pltpu.VMEM((SLOTS * T, D), BF16),
    pltpu.VMEM((SLOTS * T, D), BF16),
    pltpu.VMEM((SLOTS * T, 3 * D), BF16),
    pltpu.VMEM((SLOTS * T, D), BF16),
    pltpu.VMEM((SLOTS * HEADS // 2, T, 128), F32),
    pltpu.VMEM((SLOTS * HEADS // 2, T, 128), BF16),
    pltpu.VMEM((D, 3 * D), BF16),
    pltpu.VMEM((D, D), BF16),
    pltpu.VMEM((D, 3 * D), BF16),
    pltpu.VMEM((D, D), BF16),
    pltpu.SemaphoreType.DMA((4,)),
]


def attend_kernel(
    me_ref,
    ids_ref,
    local_ref,
    recv_ref,
    self_gain_ref,
    cross_gain_ref,
    mlp_gain_ref,
    self_qkv_hbm,
    self_out_hbm,
    cross_qkv_hbm,
    cross_out_hbm,
    after_ref,
    mlp_in_ref,
    x_ref,
    y_ref,
    qkv_ref,
    att_ref,
    score_ref,
    expo_ref,
    self_qkv,
    self_out,
    cross_qkv,
    cross_out,
    sems,
):
    side = me_ref[0] & 1
    copies = [
        pltpu.make_async_copy(src.at[side], dst, sems.at[n])
        for n, (src, dst) in enumerate(
            (
                (self_qkv_hbm, self_qkv),
                (self_out_hbm, self_out),
                (cross_qkv_hbm, cross_qkv),
                (cross_out_hbm, cross_out),
            )
        )
    ]
    copies[0].start()

    def place(first_ref, second_ref):
        first_ref[0:64] = local_ref[4]
        first_ref[64:128] = jnp.where((ids_ref[2] & 1) == side, local_ref[2], recv_ref[3])
        first_ref[128:192] = recv_ref[4]
        first_ref[192:256] = jnp.where((ids_ref[7] & 1) == side, local_ref[3], recv_ref[2])
        second_ref[0:64] = local_ref[0]
        second_ref[64:128] = local_ref[1]
        second_ref[128:192] = recv_ref[0]
        second_ref[192:256] = recv_ref[1]

    @pl.when(side == 0)
    def _():
        place(x_ref, y_ref)

    @pl.when(side == 1)
    def _():
        place(y_ref, x_ref)

    xn = normed(x_ref[...], self_gain_ref[pl.ds(side, 1), :])
    copies[0].wait()
    for copy in copies[1:]:
        copy.start()
    qkv_ref[...] = matmul(xn, self_qkv[...]).astype(BF16)
    attention(qkv_ref, score_ref, expo_ref, att_ref)
    copies[1].wait()
    after_self = (x_ref[...].astype(F32) + matmul(att_ref[...], self_out[...])).astype(BF16)
    x_ref[...] = after_self
    qn = normed(after_self, cross_gain_ref[pl.ds(2 * side, 1), :])
    yn = normed(y_ref[...], cross_gain_ref[pl.ds(2 * side + 1, 1), :])
    copies[2].wait()
    qkv_ref[:, 0:D] = matmul(qn, cross_qkv[:, 0:D]).astype(BF16)
    qkv_ref[:, D : 3 * D] = matmul(yn, cross_qkv[:, D : 3 * D]).astype(BF16)
    attention(qkv_ref, score_ref, expo_ref, att_ref)
    copies[3].wait()
    after_cross = (x_ref[...].astype(F32) + matmul(att_ref[...], cross_out[...])).astype(BF16)
    after_ref[...] = after_cross
    mlp_in_ref[...] = normed(after_cross, mlp_gain_ref[pl.ds(side, 1), :])


def gelu(v):
    return v * (lax.erf(v * 0.7071067811865476) + 1.0) * 0.5


def accumulate(groups, mlp_in_ref, weights, acc_ref, held, sems):
    copies, at = [], 0
    for n, size in enumerate(groups):
        blocks = []
        for m in range(size):
            part = slice(m * 8 // size, (m + 1) * 8 // size)
            to = held.at[n, pl.ds(part.start, part.stop - part.start)]
            blocks.append(pltpu.make_async_copy(weights[at], to, sems.at[at]))
            at += 1
        copies.append(blocks)
    for blocks in copies[:2]:
        for copy in blocks:
            copy.start()
    for n, blocks in enumerate(copies):
        for copy in blocks:
            copy.wait()
        for copy in sum(copies[n + 2 : n + 3], []):
            copy.start()
        up = held[n, :, 0].reshape(384, D)
        down = held[n, :, 1].reshape(384, D)
        lifted = lax.dot_general(
            mlp_in_ref[...], up, (((1,), (1,)), ((), ())), preferred_element_type=F32
        )
        acc_ref[...] += matmul(gelu(lifted).astype(BF16), down)


def mlp_kernel(groups, after_ref, mlp_in_ref, *refs):
    count = sum(groups)
    acc_ref, held, sems = refs[count:]
    acc_ref[...] = after_ref[...].astype(F32)
    accumulate(groups, mlp_in_ref, refs[:count], acc_ref, held, sems)


def mlp_last_kernel(groups, me_ref, ids_ref, before_ref, mlp_in_ref, conf_ref, *refs):
    count = sum(groups)
    own_ref, a_ref, b_ref, acc_ref, message, held, sems = refs[count:]
    acc_ref[...] = before_ref[...]
    accumulate(groups, mlp_in_ref, refs[:count], acc_ref, held, sems)
    decoded = acc_ref[...].astype(BF16)
    conf = 1.0 + jnp.exp(jnp.sum(decoded.astype(F32) * conf_ref[...], -1, keepdims=True))
    high = conf.astype(BF16)
    rest = conf - high.astype(F32)
    middle = rest.astype(BF16)
    low = (rest - middle.astype(F32)).astype(BF16)
    lane = lax.broadcasted_iota(jnp.int32, (T, AUX), 1)
    side = me_ref[0] & 1
    for slot in range(SLOTS):
        rows = slice(slot * T, slot * T + T)
        at = 5 * (slot // 2)
        first, second = ids_ref[at + 2 * (slot % 2)], ids_ref[at + 2 * (slot % 2) + 1]
        owner = jnp.where(slot % 2 < ids_ref[at + 4], jnp.where(side == 0, first, second), -1).astype(F32)
        aux = jnp.where(lane == 0, owner, 0.0)
        aux = jnp.where(lane == 1, high[rows].astype(F32), aux)
        aux = jnp.where(lane == 2, middle[rows].astype(F32), aux)
        aux = jnp.where(lane == 3, low[rows].astype(F32), aux)
        message[slot, :, 0:D] = decoded[rows]
        message[slot, :, D:MSG] = aux.astype(BF16)

    def put(ref, slots):
        for n, slot in enumerate(slots):
            ref[n] = message[slot]

    @pl.when(side == 0)
    def _():
        put(own_ref, (0, 2))
        put(a_ref, (1, 3))
        put(b_ref, (1, 3))

    @pl.when(side == 1)
    def _():
        put(own_ref, (0, 2))
        put(a_ref, (2, 3))
        put(b_ref, (0, 1))


def total_of(aux):
    return aux[:, 1:2] + aux[:, 2:3] + aux[:, 3:4]


def owner_of(ref, slot):
    lane = lax.broadcasted_iota(jnp.int32, (16, AUX), 1)
    aux = ref[slot, 0:16, D:MSG].astype(F32)
    return jnp.max(jnp.where(lane == 0, aux, -1.0)).astype(jnp.int32)


def add_to(sums, ref, slot):
    conf = total_of(ref[slot, :, D:MSG].astype(F32))
    sums[:, 0:D] += conf * ref[slot, :, 0:D].astype(F32)
    sums[:, D:MSG] += jnp.broadcast_to(conf, (T, AUX))


def load(sources, held, sems):
    copies = [
        pltpu.make_async_copy(src, held.at[pl.ds(2 * n, 2)], sems.at[n]) for n, src in enumerate(sources)
    ]
    for copy in copies:
        copy.start()
    return copies


def middle_kernel(me_ref, *refs):
    out_0 = refs[8]
    outs = refs[9:12]
    sums, held, sems = refs[12:]
    z, x, _, core = coordinates(me_ref[0])

    @pl.when(core == 0)
    def _():
        load(refs[0:4], held, sems)

    @pl.when(core == 1)
    def _():
        load(refs[4:8], held, sems)

    copies = [pltpu.make_async_copy(refs[n], held.at[pl.ds(2 * n, 2)], sems.at[n]) for n in range(4)]
    sums[0:4] = jnp.zeros((4, T, MSG), F32)
    for n in range(8):
        if n % 2 == 0:
            copies[n // 2].wait()
        owner = owner_of(held, n)
        to_z, to_x, _, _ = coordinates(owner)
        here = jnp.where(core == 0, to_x == x, to_z == z)
        to = jnp.where(core == 0, to_z ^ z, to_x ^ x)
        add_to(sums.at[jnp.where((owner >= 0) & here, to, 4)], held, n)

    out_0[...] = sums[0]
    lane = lax.broadcasted_iota(jnp.int32, (T, AUX), 1)
    for mask, out in zip((1, 3, 2), outs):
        out[:, 0:D] = sums[mask, :, 0:D].astype(BF16)
        denominator = sums[mask, :, D:MSG]
        high = denominator.astype(BF16)
        rest = denominator - high.astype(F32)
        middle = rest.astype(BF16)
        low = rest - middle.astype(F32)
        aux = jnp.where(lane == 1, high.astype(F32), 0.0)
        aux = jnp.where(lane == 2, middle.astype(F32), aux)
        out[:, D:MSG] = jnp.where(lane == 3, low, aux).astype(BF16)


def row_kernel(me_ref, *refs):
    mine, theirs, held, sems = refs[5:]
    me = me_ref[0]
    mine[...] = jnp.zeros((T, MSG), F32)
    theirs[...] = jnp.zeros((T, MSG), F32)

    @pl.when((me & 1) == 0)
    def _():
        copies = load(refs[:5], held, sems)
        for n in range(10):
            if n % 2 == 0:
                copies[n // 2].wait()
            owner = owner_of(held, n)

            @pl.when(owner == me)
            def _(n=n):
                add_to(mine, held, n)

            @pl.when(owner == me + 1)
            def _(n=n):
                add_to(theirs, held, n)


def final_kernel(me_ref, column, row, row_there, from_1, from_3, from_2, head, out_ref):
    sums = column[...] + jnp.where((me_ref[0] & 1) == 0, row[...], row_there[...])
    numerator, denominator = sums[:, 0:D], sums[:, D : D + 1]
    for piece in (from_1, from_3, from_2):
        numerator += piece[:, 0:D].astype(F32)
        denominator += total_of(piece[:, D:MSG].astype(F32))
    joined = (numerator / denominator).astype(BF16)
    out_ref[0] = matmul(joined, head[...]).astype(BF16)


def params(mib):
    return pltpu.CompilerParams(vmem_limit_bytes=mib * 2**20)


def shards(
    encoder_tokens,
    pair_list,
    pair_count,
    embed_weight,
    self_gain,
    self_qkv,
    self_out,
    cross_gain,
    cross_qkv,
    cross_out,
    mlp_gain,
    mlp_up,
    mlp_down,
    conf_weight,
    head_weight,
):
    me = lax.axis_index("row") * 8 + lax.axis_index("col")
    core = me & 1

    up_out, down_out = (lax.dynamic_index_in_dim(w, 1 - core, 0, False) for w in (mlp_up, mlp_down))
    came = swap(jnp.stack([up_out, down_out]))
    up_own, down_own = (lax.dynamic_index_in_dim(w, core, 0, False) for w in (mlp_up, mlp_down))
    mine = jnp.concatenate([pair_list.reshape(4), pair_count.reshape(1)])
    theirs = swap(mine)
    far = send(mine, ((Z, 1),), ((X, 1),))
    ids = (me.reshape(1), jnp.concatenate([mine, theirs]))

    own = jnp.einsum(
        "td,de->te", encoder_tokens[0], embed_weight, preferred_element_type=F32
    ).astype(BF16)

    block = jnp.concatenate([jnp.stack([up_own, down_own]), came], axis=1)
    block = join(block.reshape(96, D), own)[None]
    line = join(block, send(block, ((Y, 1),), ((Y, 3),)))
    line_far = send(line, ((Y, 3),), ((Y, 1),))

    def over_plane(held, first, last, one, two):
        near = send(held, ((first, 1),), ((first, 3),))
        held = join(held[:, :96], near[:, :96])
        held = join(held, send(held, ((first, 3),), ((first, 1),)))
        near = send(held, ((last, one),), ((last, two),))
        half = lax.dynamic_slice_in_dim(held, ((me >> 1) & 1) * 4, 4, 0)
        far = send(half, ((last, two),), ((last, one),))
        rest = send(far, ((Y, 1),), ((Y, 3),))
        across = send(near, ((last, two),), ((last, one),))
        return [h.reshape(-1, 2, 48, D) for h in (held, near, far, rest, across)]

    weights_a = over_plane(line, X, Z, 3, 1)
    weights_b = over_plane(line_far, Z, X, 1, 3)

    tokens = own[None]
    tokens = join(tokens, send(tokens, ((X, 1),), ((Z, 1),)))
    tokens = join(tokens, send(tokens, ((X, 3),), ((Z, 3),)))
    tokens = join(tokens, send(tokens, ((Z, 3),), ((X, 3),)))
    picked = pl.pallas_call(
        pick_kernel,
        out_shape=jax.ShapeDtypeStruct((2, T, D), BF16),
        in_specs=[SMEM] * 2 + [HBM],
        out_specs=VMEM,
        scratch_shapes=[pltpu.SemaphoreType.DMA((2,))],
        name="pick",
    )(ids[0], far, *in_hbm(tokens))
    tokens_far = send(picked, ((Z, 1),), ((X, 1),))
    selected = pl.pallas_call(
        select_kernel,
        out_shape=jax.ShapeDtypeStruct((5, T, D), BF16),
        in_specs=[SMEM] * 2 + [HBM] * 4 + [VMEM],
        out_specs=VMEM,
        scratch_shapes=[pltpu.SemaphoreType.DMA((4,))],
        name="select",
    )(*ids, *in_hbm(tokens, tokens_far, line, line_far), own)
    received = swap(selected)

    after, mlp_in = pl.pallas_call(
        attend_kernel,
        out_shape=[jax.ShapeDtypeStruct((SLOTS * T, D), BF16)] * 2,
        in_specs=[SMEM] * 2 + [VMEM] * 5 + [HBM] * 4,
        out_specs=[VMEM, VMEM],
        scratch_shapes=ATT_SCRATCH,
        compiler_params=params(32),
        name="attend",
    )(
        *ids,
        selected,
        received,
        self_gain,
        cross_gain.reshape(4, D),
        mlp_gain,
        *in_hbm(self_qkv, self_out, cross_qkv, cross_out),
    )

    def held_weights(groups):
        return [pltpu.VMEM((len(groups), 8, 2, 48, D), BF16), pltpu.SemaphoreType.DMA((sum(groups),))]

    early, late = (1, 1, 1, 1, 2), (2, 1, 1)

    sums = jax.ShapeDtypeStruct((SLOTS * T, D), F32)
    partial = pl.pallas_call(
        functools.partial(mlp_kernel, early),
        out_shape=sums,
        in_specs=[VMEM] * 2 + [HBM] * sum(early),
        out_specs=VMEM,
        scratch_shapes=held_weights(early),
        compiler_params=params(32),
        name="lift",
    )(
        after,
        mlp_in,
        *(weights_a[0], weights_b[0], weights_a[1], weights_b[1], weights_a[2], weights_a[3]),
    )
    msg = lambda *shape: jax.ShapeDtypeStruct((*shape, MSG), BF16)
    piece_own, piece_a, piece_b = pl.pallas_call(
        functools.partial(mlp_last_kernel, late),
        out_shape=[msg(2, T)] * 3,
        in_specs=[SMEM] * 2 + [VMEM] * 3 + [HBM] * sum(late),
        out_specs=[VMEM] * 3,
        scratch_shapes=[pltpu.VMEM((SLOTS * T, D), F32), pltpu.VMEM((SLOTS, T, MSG), BF16)]
        + held_weights(late),
        compiler_params=params(32),
        name="last",
    )(
        *ids,
        partial,
        mlp_in,
        conf_weight.reshape(1, D),
        *(weights_b[2], weights_b[3], weights_a[4], weights_b[4]),
    )

    masks = (1, 3, 2)
    got_a = [swap(piece_a)]
    got_a += [send(piece_a, ((C, 1),), ((X, m), (C, 1))) for m in masks]
    got_b = [send(piece_b, ((Y, m),), ((Z, m),)) for m in masks]
    pieces = in_hbm(*got_a, piece_b, *got_b)
    summed = jax.ShapeDtypeStruct((T, MSG), F32)
    column, *parts = pl.pallas_call(
        middle_kernel,
        out_shape=[summed] + [msg(T)] * 3,
        in_specs=[SMEM] + [HBM] * 8,
        out_specs=[VMEM] * 4,
        scratch_shapes=[
            pltpu.VMEM((5, T, MSG), F32),
            pltpu.VMEM((8, T, MSG), BF16),
            pltpu.SemaphoreType.DMA((4,)),
        ],
        name="middle",
    )(ids[0], *pieces)
    last = [send(s, ((Z, m),), ((X, m),)) for s, m in zip(parts, masks)]
    row, row_out = pl.pallas_call(
        row_kernel,
        out_shape=[summed] * 2,
        in_specs=[SMEM] + [HBM] * 5,
        out_specs=[VMEM] * 2,
        scratch_shapes=[pltpu.VMEM((10, T, MSG), BF16), pltpu.SemaphoreType.DMA((5,))],
        name="rows",
    )(ids[0], *in_hbm(piece_own), *pieces[4:])
    row_there = swap(row_out)
    return pl.pallas_call(
        final_kernel,
        out_shape=jax.ShapeDtypeStruct((1, T, 1024), BF16),
        in_specs=[SMEM] + [VMEM] * 7,
        out_specs=VMEM,
        name="head",
    )(ids[0], column, row, row_there, *last, head_weight)


def solution(mesh):
    return jax.shard_map(
        shards,
        mesh=mesh,
        in_specs=(
            P(("row", "col"), None, None),
            P("row", "col", None, None),
            P("row", "col"),
            P(),
            P(),
            P(),
            P(),
            P(),
            P(),
            P(),
            P(),
            P(None, ("row", "col"), None),
            P(None, ("row", "col"), None),
            P(),
            P(),
        ),
        out_specs=P(("row", "col"), None, None),
        check_vma=False,
    )
```
